128 devices in a mesh: section: 4 (over y_hi, core), fsdp: 32 (over y_lo, x, z).
Axes of the slice: x: 4, y: 4 (y_hi: 2, y_lo: 2; y = y_hi * 2 + y_lo), z: 4, core: 2. Of those that a mesh axis runs over, the one named last changes fastest.
Arguments:
- old_pieces: bfloat16 [4, 2, 16384, 1024], P('section', None, 'fsdp'), may hold values from -0.0625 to 0.0625
- section_inputs: bfloat16 [4, 16384, 8192], P('section', 'fsdp'), may hold values from -6 to 6
- old_section_of: int32 [8], replicated, may hold values from 0 to 3, as said below
- new_section_of: int32 [8], replicated, may hold values from 0 to 7, as said below
- old_order: int32 [8, 2], replicated, may hold values from 0 to 1, each once within a row
- new_order: int32 [8, 2], replicated, may hold values from 0 to 1, each once within a row
Outputs:
- new_shards: bfloat16 [4, 32768, 1024], P('section', 'fsdp')
- kv_out: bfloat16 [4, 16384, 2048], P('section', 'fsdp')
The draws below stay inside these ranges and needn't reach their ends.
Inputs may be any that keep to these rules, and one draw needn't show every extreme that they name: `old_section_of`: each old section holds exactly two layers. Each new section holds exactly one layer; the two layers of one old section have different values of new_section_of // 2.
All inputs are finite; a program needn't handle non-finite values.
Results may differ from the reference program's by a relative error of at most 0.001.
Values may be sent and summed in bfloat16 or wider, within the bound.
A program may use at most 192 MiB of HBM per device.

```python
import math
import jax
import jax.numpy as jnp
from jax import lax

D = 8192
HEAD_DIM = 128
TOK_DEV = 512
KVW = 1024
LAYERS = 8
SHARD = 1024
N_SECTION = 4
N_FSDP = 32


def layer_maps(key):
    section_count = N_SECTION
    keys = jax.random.split(jax.random.fold_in(key, 11), 6)
    members = jax.random.permutation(keys[0], 2 * section_count).astype(jnp.int32)
    old_section = (jnp.argsort(members) // 2).astype(jnp.int32)
    rows_first = jax.random.permutation(keys[1], section_count).astype(jnp.int32)
    relabel = jax.random.permutation(keys[2], section_count).astype(jnp.int32)
    offset_steps = jax.random.randint(keys[3], (), 1, section_count).astype(jnp.int32)
    relabel_inverse = jnp.argsort(relabel).astype(jnp.int32)
    rows_second = rows_first[relabel_inverse[(relabel + offset_steps) % section_count]]
    swapped = jax.random.randint(keys[4], (section_count,), 0, 2).astype(jnp.int32)
    layer_alpha = jnp.where(swapped == 0, members[0::2], members[1::2])
    layer_beta = jnp.where(swapped == 0, members[1::2], members[0::2])
    halves = jax.random.randint(keys[5], (section_count,), 0, 2).astype(jnp.int32)
    section_alpha = 2 * rows_first + halves[rows_first]
    section_beta = 2 * rows_second + 1 - halves[rows_second]
    new_section = jnp.zeros((2 * section_count,), jnp.int32).at[layer_alpha].set(section_alpha).at[layer_beta].set(section_beta)
    return (old_section, new_section)


def draw_old_section_of(key, part):
    return layer_maps(key)[0]


def draw_new_section_of(key, part):
    return layer_maps(key)[1]


def levels(stream_key, dims, shards, low, high):
    factor_of = 1.0
    for dim, parts in shards:
        heights = jax.random.uniform(jax.random.fold_in(jax.random.fold_in(stream_key, 6), dim), (parts,), jnp.float32, low / len(shards), high / len(shards))
        factor_of = factor_of * jnp.repeat(jnp.exp(heights), dims[dim] // parts).reshape((-1,) + (1,) * (len(dims) - 1 - dim))
    return factor_of


def noise(key, extent, deviation, most, shards=(), kind=jnp.bfloat16):
    level = levels(key, extent, shards, -0.22, 0.18) if shards else 1.0
    result = jax.random.normal(key, extent, jnp.float32) * deviation * level
    return jnp.minimum(jnp.maximum(result, -most), most).astype(kind)


def setup_inputs(seed: int = 0) -> dict:
    streams_of = jax.random.split(jax.random.key(seed), 7)
    return {
        "old_pieces": noise(streams_of[0], (N_SECTION, 2, 2 * D, KVW), D ** -0.5, 0.0625, ((0, 4), (2, 32))),
        "section_inputs": noise(streams_of[1], (N_SECTION, N_FSDP * TOK_DEV, D), 1.0, 6.0, ((0, 4), (1, 32))),
        "old_section_of": draw_old_section_of(jax.random.fold_in(streams_of[6], 71), 0),
        "new_section_of": draw_new_section_of(jax.random.fold_in(streams_of[6], 71), 0),
        "old_order": jax.vmap(lambda own: jax.random.permutation(own, 2))(jax.random.split(streams_of[4], LAYERS)).reshape((LAYERS, 2)).astype(jnp.int32),
        "new_order": jax.vmap(lambda own: jax.random.permutation(own, 2))(jax.random.split(streams_of[5], LAYERS)).reshape((LAYERS, 2)).astype(jnp.int32),
    }


def rotate_keys(values, positions):
    tok_rows = values.shape[0]
    heads = values.reshape(tok_rows, -1, HEAD_DIM)
    half_dim = HEAD_DIM // 2
    freq_index = jnp.arange(half_dim, dtype=jnp.float32)
    inverse_freq = jnp.exp(freq_index * (-2.0 * math.log(500000.0) / HEAD_DIM))
    angles = positions.astype(jnp.float32)[:, None] * inverse_freq[None, :]
    cosine = jnp.cos(angles)[:, None, :]
    sine = jnp.sin(angles)[:, None, :]
    lower = heads[..., :half_dim]
    upper = heads[..., half_dim:]
    turned = jnp.concatenate([lower * cosine - upper * sine, upper * cosine + lower * sine], axis=-1)
    return turned.reshape(tok_rows, -1)


def reference(old_pieces, section_inputs, old_section_of, new_section_of, old_order, new_order):
    layer_ids = jnp.arange(LAYERS, dtype=jnp.int32)
    group_size = N_FSDP // 2
    shard_list = []
    output_list = []
    for row_index in range(N_SECTION):
        shard_halves = []
        output_halves = []
        for half in range(2):
            layer_index = jnp.sum(jnp.where(new_section_of == 2 * row_index + half, layer_ids, 0)).astype(jnp.int32)
            old_section = old_section_of[layer_index]
            slot_index = jnp.sum(((old_section_of == old_section) & (layer_ids < layer_index)).astype(jnp.int32))
            flat_rows = old_pieces[old_section, slot_index]
            key_weight = lax.dynamic_slice_in_dim(flat_rows, (old_order[layer_index, 0] * D).astype(jnp.int32), D, 0)
            value_weight = lax.dynamic_slice_in_dim(flat_rows, (old_order[layer_index, 1] * D).astype(jnp.int32), D, 0)
            new_flat = jnp.where(new_order[layer_index, 0] == 0,
                                 jnp.concatenate([key_weight, value_weight], axis=0),
                                 jnp.concatenate([value_weight, key_weight], axis=0))
            shard_halves.append(new_flat.reshape(group_size, SHARD, KVW))
            tokens = section_inputs[row_index].reshape(group_size, 2, TOK_DEV, D)[:, half].reshape(group_size * TOK_DEV, D)
            keys = jnp.dot(tokens, key_weight, preferred_element_type=jnp.float32)
            values = jnp.dot(tokens, value_weight, preferred_element_type=jnp.float32)
            positions = jnp.arange(group_size * TOK_DEV, dtype=jnp.int32)
            joined = jnp.concatenate([rotate_keys(keys, positions), values], axis=-1).astype(jnp.bfloat16)
            output_halves.append(joined.reshape(group_size, TOK_DEV, 2 * KVW))
        shard_list.append(jnp.stack(shard_halves, axis=1).reshape(4 * D, KVW))
        output_list.append(jnp.stack(output_halves, axis=1).reshape(N_FSDP * TOK_DEV, 2 * KVW))
    return jnp.stack(shard_list), jnp.stack(output_list)
```

```python
import math

import jax
import jax.numpy as jnp
from jax import lax
from jax.experimental import pallas as pl
from jax.experimental.pallas import tpu as pltpu
from jax.sharding import PartitionSpec as P

HEAD_DIM = 128
MESH = pl.DeviceIdType.MESH
NC = 8
NG = 4
TU = 8


def body(oldsec, newsec, oldord, neword, pieces, tokens, cos_in, sin_in, kv_out, shard_out,
         pc, og, cand, tb, sf, wb, n2, sha, shb, xb, acc, ob, ct, st,
         pc_sem, rs, rr, ws, wr, zs, zr, xs, xr, ns, nr, shl, shs, shr,
         tl, tas, tar, ts, tr, tfs, tfr, osm, orm, olm, tab_sem):
    rows = pieces.shape[1]
    cw = pieces.shape[2] // NC
    gw = pieces.shape[2] // NG
    per = NC // NG
    tok_rows, width = tokens.shape
    layers = oldsec.shape[0]
    s = lax.axis_index("section")
    m = lax.axis_index("fsdp")
    y = s // 2
    c = s % 2
    j = m // 16
    x = (m // 4) % 4
    z = m % 4
    h = z % 2
    is_a = c == j
    is_b = c != j

    def dev(yy, cc, jj, xx, zz):
        return (2 * yy + cc, jj * 16 + xx * 4 + zz)

    core_dev = dev(y, 1 - c, j, x, z)
    cross_dev = [dev(1 - y, k, 1 - j, x, z) for k in range(2)]
    side_dev = [dev(y, k, 1 - j, x, z) for k in range(2)]
    zp, zm, zf = (z + 1) % 4, (z + 3) % 4, (z + 2) % 4
    xp, xm, xf = (x + 1) % 4, (x + 3) % 4, (x + 2) % 4
    zp_dev, zm_dev, zf_dev = (dev(y, c, j, x, zz) for zz in (zp, zm, zf))
    xp_dev, xm_dev = (dev(y, c, j, xx, z) for xx in (xp, xm))

    def remote(src, dst, send, recv, device):
        return pltpu.make_async_remote_copy(
            src_ref=src, dst_ref=dst, send_sem=send, recv_sem=recv,
            device_id=device, device_id_type=MESH)

    def arrived(dst, send, recv, device):
        remote(dst, dst, send, recv, device).wait_recv()

    def pc_copy(i, a):
        return pltpu.make_async_copy(
            pieces.at[a, :, pl.ds(i * cw, cw)], pc.at[i, a], pc_sem.at[i, a])

    for i in range(NC):
        for a in range(2):
            pc_copy(i, a).start()
    table_copies = [pltpu.make_async_copy(cos_in, ct, tab_sem.at[0]),
                    pltpu.make_async_copy(sin_in, st, tab_sem.at[1])]
    for copy in table_copies:
        copy.start()

    def layer_of(section):
        found = jnp.int32(0)
        for l in range(layers):
            found = found + jnp.where(newsec[l] == section, l, 0)
        return found

    def entry(table, layer):
        found = jnp.int32(0)
        for l in range(layers):
            found = found + jnp.where(layer == l, table(l), 0)
        return found

    high = jnp.int32(0)
    for l in range(layers):
        high = jnp.where(oldsec[l] == s, l, high)
    row_high = entry(lambda l: newsec[l], high) // 2
    source = [entry(lambda l: oldsec[l], layer_of(2 * s + k)) for k in range(2)]
    source_own = jnp.where(h == 0, source[0], source[1])
    source_other = jnp.where(h == 0, source[1], source[0])
    gl = layer_of(2 * (2 * y + j) + h)
    gl_crossed = jnp.where(entry(lambda l: oldsec[l], gl) // 2 == y, 0, 1)
    gl_old = entry(lambda l: oldord[2 * l], gl)
    gl_new = entry(lambda l: neword[2 * l], gl)
    gl_turn = (jnp.where(gl_old == gl_new, 0, 1) + gl_crossed) % 2
    is_key = gl_old == (c + gl_crossed) % 2

    barrier = pltpu.get_barrier_semaphore()
    partners = [core_dev] + cross_dev + side_dev + [zp_dev, zm_dev, zf_dev, xp_dev, xm_dev]
    for device in partners:
        pl.semaphore_signal(barrier, inc=1, device_id=device, device_id_type=MESH)
    pl.semaphore_wait(barrier, len(partners))

    tok_step = width // (2 * TU)
    quarter = width // 4

    def tok_send(v):
        u, a = v // 2, v % 2
        cols = pl.ds((a * TU + u) * tok_step, tok_step)
        return remote(tokens.at[:, cols], xb.at[1, :, cols], ts.at[v], tr.at[u], side_dev[a])

    def tok_here(u):
        cols = pl.ds(pl.multiple_of((c * TU + u) * tok_step, 128), tok_step)
        return remote(xb.at[1, :, cols], xb.at[1, :, cols], tfs.at[u], tr.at[u], core_dev)

    def tok_pass(u):
        cols = pl.ds(pl.multiple_of((c * TU + u) * tok_step, 128), tok_step)
        return remote(xb.at[1, :, cols], xb.at[1, :, cols], tfs.at[u], tfr.at[u], core_dev)

    def tok_other(u):
        cols = pl.ds(pl.multiple_of(((1 - c) * TU + u) * tok_step, 128), tok_step)
        return remote(xb.at[1, :, cols], xb.at[1, :, cols], tfs.at[u], tfr.at[u], core_dev)

    def tok_core(k):
        cols = pl.ds(k * quarter, quarter)
        return remote(tokens.at[:, cols], xb.at[0, :, cols], tas.at[k], tar.at[k], core_dev)

    tok_local = pltpu.make_async_copy(tokens, xb.at[0], tl.at[0])
    tok_next = [0]

    def send_tokens(count):
        take = range(tok_next[0], min(tok_next[0] + count, 2 * TU))
        tok_next[0] += len(take)

        @pl.when(is_b)
        def _():
            for v in take:
                tok_send(v).start()

    def relay_copies(i):
        return [remote(og.at[i, k], cand.at[i, s], rs.at[i, k],
                       rr.at[i, 0] if k == 0 else rr.at[i, 1 + c], device)
                for k, device in enumerate([core_dev] + cross_dev)]

    relay_rows = [2 * y + 1 - c, 2 * (1 - y), 2 * (1 - y) + 1]

    def relay_send(i):
        for a in range(2):
            pc_copy(i, a).wait()

        def tile(t, carry):
            part = pl.ds(pl.multiple_of(t * 128, 128), 128)
            low_rows = pc[i, 0, part, :]
            high_rows = pc[i, 1, part, :]
            for k in range(3):
                og[i, k, part, :] = jnp.where(row_high == relay_rows[k], high_rows, low_rows)
            cand[i, s, part, :] = jnp.where(row_high == s, high_rows, low_rows)
            return carry

        lax.fori_loop(0, rows // 128, tile, 0)
        for copy in relay_copies(i):
            copy.start()

    place = pl.ds(pl.multiple_of((x * 4 + z) * rows, rows), rows)

    def swap_copies(i):
        device = dev(y, 1 - c, 1 - j, x, z)
        return [remote(tb.at[i, 0], wb.at[i, place], ws.at[i, 0], wr.at[i, 0], device),
                remote(tb.at[i, 1], sf.at[i], ws.at[i, 1], wr.at[i, 1], device)]

    def choose(i):
        arrived(cand.at[i, 2 * y + 1 - c], rs.at[i, 0], rr.at[i, 0], core_dev)
        for k in range(2):
            arrived(cand.at[i, 2 * (1 - y) + k], rs.at[i, 1 + k], rr.at[i, 1 + k], cross_dev[k])

        def picked(part):
            four = [cand[i, k, part, :] for k in range(4)]
            out = []
            for want in (source_own, source_other):
                out.append(jnp.where(want < 2, jnp.where(want == 0, four[0], four[1]),
                                     jnp.where(want == 2, four[2], four[3])))
            return out

        @pl.when(is_a)
        def _():
            def tile(t, carry):
                part = pl.ds(pl.multiple_of(t * 128, 128), 128)
                mine, other = picked(part)
                wb[i, pl.ds(pl.multiple_of((x * 4 + z) * rows + t * 128, 128), 128), :] = mine
                sf[i, part, :] = other
                return carry

            lax.fori_loop(0, rows // 128, tile, 0)

        @pl.when(is_b)
        def _():
            def tile(t, carry):
                part = pl.ds(pl.multiple_of(t * 128, 128), 128)
                mine, other = picked(part)
                tb[i, 0, part, :] = mine
                tb[i, 1, part, :] = other
                return carry

            lax.fori_loop(0, rows // 128, tile, 0)
            for copy in swap_copies(i):
                copy.start()

    def z_copies(i):
        return [remote(sf.at[i], wb.at[i, place], zs.at[i, 0], zr.at[i, 0], zp_dev),
                remote(sf.at[i], wb.at[i, place], zs.at[i, 1], zr.at[i, 1], zm_dev),
                remote(wb.at[i, place], wb.at[i, place], zs.at[i, 2], zr.at[i, 2], zf_dev)]

    def z_send(i):
        @pl.when(is_b)
        def _():
            for copy in swap_copies(i):
                copy.wait_recv()
        for copy in z_copies(i):
            copy.start()

    def block(i, xx, first, count):
        return wb.at[i, pl.ds(pl.multiple_of(xx * 4 * rows + first, rows), count)]

    def own_copies(i):
        mine = block(i, x, 0, 4 * rows)
        return [remote(mine, mine, xs.at[i, 0], xr.at[i, 0], xp_dev),
                remote(mine, mine, xs.at[i, 1], xr.at[i, 1], xm_dev)]

    def pass_copies(i):
        left = block(i, xm, 0, 2 * rows)
        right = block(i, xp, 2 * rows, 2 * rows)
        return [remote(left, left, xs.at[i, 2], xr.at[i, 2], xp_dev),
                remote(right, right, xs.at[i, 3], xr.at[i, 3], xm_dev)]

    pair = pl.ds(pl.multiple_of((x * 4 + z // 2 * 2) * rows, rows), 2 * rows)

    def near_copy(i):
        return remote(wb.at[i, pair], n2.at[i], ns.at[i], nr.at[i], core_dev)

    def x_own(i):
        for k, zz in enumerate((zm, zp, zf)):
            arrived(block(i, x, zz * rows, rows), zs.at[i, k], zr.at[i, k], zf_dev)
        for copy in own_copies(i):
            copy.start()

        @pl.when(is_b)
        def _():
            near_copy(i).start()

    def x_pass(i):
        arrived(block(i, xm, 0, 4 * rows), xs.at[i, 0], xr.at[i, 0], xp_dev)
        first, second = pass_copies(i)
        first.start()
        arrived(block(i, xp, 0, 4 * rows), xs.at[i, 1], xr.at[i, 1], xm_dev)
        second.start()

    def far_arrived(i):
        arrived(block(i, xf, 0, 2 * rows), xs.at[i, 2], xr.at[i, 2], xp_dev)
        arrived(block(i, xf, 2 * rows, 2 * rows), xs.at[i, 3], xr.at[i, 3], xm_dev)

    def shard_local(i):
        return pltpu.make_async_copy(sha.at[i], shard_out.at[:, pl.ds(i * cw, cw)], shl.at[i])

    def shard_far(i):
        return remote(shb.at[i], shard_out.at[:, pl.ds(i * cw, cw)], shs.at[i], shr.at[i],
                      dev(y, c, 1 - j, x, z))

    def shard(i):
        @pl.when(is_a)
        def _():
            near_copy(i).wait_recv()

            def tile(t, carry):
                part = pl.ds(pl.multiple_of(t * 128, 128), 128)
                near = pl.ds(pl.multiple_of((x * 4 + z // 2 * 2) * rows + t * 128, 128), 128)
                mine = wb[i, near, :]
                other = n2[i, part, :]
                sha[i, part, :] = jnp.where(gl_turn == 0, mine, other)
                shb[i, part, :] = jnp.where(gl_turn == 0, other, mine)
                return carry

            lax.fori_loop(0, 2 * rows // 128, tile, 0)

    def shard_send(i):
        @pl.when(is_a)
        def _():
            shard_local(i).start()
            shard_far(i).start()

    def multiply(g, xx, half):
        first = pl.multiple_of(xx * 4 * rows + half * 2 * rows, 2 * rows)
        ks = pl.ds(first, 2 * rows)
        weight = jnp.concatenate([wb[per * g + k, ks, :] for k in range(per)], axis=1)
        for slot in range(2):
            acc[slot] += jnp.dot(xb[slot, :, ks], weight, preferred_element_type=jnp.float32)

    def finish(g):
        def tile(t, carry):
            part = pl.ds(pl.multiple_of(t * 64, 64), 64)
            for slot in range(2):
                cosine = ct[slot, part, :]
                sine = st[slot, part, :]
                for head in range(gw // HEAD_DIM):
                    cols = slice(head * HEAD_DIM, (head + 1) * HEAD_DIM)
                    value = acc[slot, part, cols]
                    turned = value * cosine + pltpu.roll(value, HEAD_DIM // 2, 1) * sine
                    ob[g, slot, part, cols] = turned.astype(jnp.bfloat16)
            return carry

        lax.fori_loop(0, tok_rows // 64, tile, 0)

    def out_local(g):
        return pltpu.make_async_copy(
            ob.at[g, 0], kv_out.at[c, :, pl.ds(g * gw, gw)], olm.at[g])

    def out_near(g):
        return remote(ob.at[g, 0], kv_out.at[c, :, pl.ds(g * gw, gw)],
                      osm.at[g, 0], orm.at[g, c], core_dev)

    def out_far(g):
        return remote(ob.at[g, 1], kv_out.at[c, :, pl.ds(g * gw, gw)],
                      osm.at[g, 1], orm.at[g, c], dev(y, j, 1 - j, x, z))

    def out_send(g):
        out_far(g).start()

        @pl.when(is_a)
        def _():
            out_local(g).start()

        @pl.when(is_b)
        def _():
            out_near(g).start()

    send_tokens(1)
    for i in range(NC):
        relay_send(i)

    @pl.when(is_a)
    def _():
        tok_local.start()
        for k in range(4):
            tok_core(k).start()

    for copy in table_copies:
        copy.wait()

    def table_tile(t, carry):
        part = pl.ds(pl.multiple_of(t * 64, 64), 64)
        for slot in range(2):
            ct[slot, part, :] = jnp.where(is_key, ct[slot, part, :], 1.0)
            st[slot, part, :] = jnp.where(is_key, st[slot, part, :], 0.0)
        return carry

    lax.fori_loop(0, tok_rows // 64, table_tile, 0)

    choose(0)
    send_tokens(1)
    for i in range(NC):
        z_send(i)
        if i + 1 < NC:
            choose(i + 1)
            send_tokens(1)
        x_own(i)
    send_tokens(2 * TU)
    for i in range(NC):
        x_pass(i)
        shard(i)
        if i < TU:
            tok_here(i).wait_recv()
            tok_pass(i).start()
    for i in range(NC):
        shard_send(i)

    @pl.when(is_a)
    def _():
        tok_local.wait()

    @pl.when(is_b)
    def _():
        for k in range(4):
            tok_core(k).wait_recv()

    for u in range(TU):
        tok_other(u).wait_recv()

    for g in range(NG):
        acc[...] = jnp.zeros_like(acc)

        def near_block(t, carry):
            b = t // 2
            multiply(g, (x + b + b // 2) % 4, t % 2)
            return carry

        lax.fori_loop(0, 6, near_block, 0)
        for k in range(per):
            far_arrived(per * g + k)

        def far_block(t, carry):
            multiply(g, xf, t)
            return carry

        lax.fori_loop(0, 2, far_block, 0)
        finish(g)
        out_send(g)

    for i in range(NC):
        for copy in relay_copies(i) + z_copies(i) + own_copies(i) + pass_copies(i):
            copy.wait_send()

    @pl.when(is_a)
    def _():
        for k in range(4):
            tok_core(k).wait_send()
        for i in range(NC):
            shard_local(i).wait()
            shard_far(i).wait_send()
        for g in range(NG):
            out_local(g).wait()
            arrived(kv_out.at[1 - c, :, pl.ds(g * gw, gw)], osm.at[g, 0], orm.at[g, 1 - c], core_dev)

    @pl.when(is_b)
    def _():
        for v in range(2 * TU):
            tok_send(v).wait_send()
        for i in range(NC):
            for copy in swap_copies(i):
                copy.wait_send()
            near_copy(i).wait_send()
            shard_far(i).wait_recv()
        for g in range(NG):
            out_near(g).wait_send()
            for k in range(2):
                arrived(kv_out.at[k, :, pl.ds(g * gw, gw)], osm.at[g, 0], orm.at[g, k], side_dev[k])

    for u in range(TU):
        tok_pass(u).wait_send()
    for g in range(NG):
        out_far(g).wait_send()


def per_device(old_pieces, section_inputs, old_section_of, new_section_of, old_order, new_order):
    s = lax.axis_index("section")
    m = lax.axis_index("fsdp")
    pieces = old_pieces[0]
    tokens = section_inputs[0]
    _, rows, kv_width = pieces.shape
    tok_rows, width = tokens.shape
    layers = old_section_of.shape[0]
    cw, gw = kv_width // NC, kv_width // NG

    half_dim = HEAD_DIM // 2
    first = jnp.stack([m // 2 * tok_rows, (m // 2 + 8) % 16 * tok_rows])
    positions = first[:, None] + jnp.arange(tok_rows, dtype=jnp.int32)[None, :]
    freq_index = jnp.arange(half_dim, dtype=jnp.float32)
    inverse_freq = jnp.exp(freq_index * (-2.0 * math.log(500000.0) / HEAD_DIM))
    angles = positions.astype(jnp.float32)[:, :, None] * inverse_freq[None, None, :]
    cosine, sine = jnp.cos(angles), jnp.sin(angles)
    cos_in = jnp.concatenate([cosine, cosine], axis=-1)
    sin_in = jnp.concatenate([-sine, sine], axis=-1)

    dma = pltpu.SemaphoreType.DMA
    bf, fl = jnp.bfloat16, jnp.float32
    hbm = pl.BlockSpec(memory_space=pltpu.HBM)
    smem = pl.BlockSpec(memory_space=pltpu.SMEM)
    kv, shards = pl.pallas_call(
        body,
        out_shape=(jax.ShapeDtypeStruct((2, tok_rows, kv_width), bf),
                   jax.ShapeDtypeStruct((2 * rows, kv_width), bf)),
        in_specs=[smem] * 4 + [hbm] * 4,
        out_specs=(hbm, hbm),
        scratch_shapes=[
            pltpu.VMEM((NC, 2, rows, cw), bf),
            pltpu.VMEM((NC, 3, rows, cw), bf),
            pltpu.VMEM((NC, 4, rows, cw), bf),
            pltpu.VMEM((NC, 2, rows, cw), bf),
            pltpu.VMEM((NC, rows, cw), bf),
            pltpu.VMEM((NC, width, cw), bf),
            pltpu.VMEM((NC, 2 * rows, cw), bf),
            pltpu.VMEM((NC, 2 * rows, cw), bf),
            pltpu.VMEM((NC, 2 * rows, cw), bf),
            pltpu.VMEM((2, tok_rows, width), bf),
            pltpu.VMEM((2, tok_rows, gw), fl),
            pltpu.VMEM((NG, 2, tok_rows, gw), bf),
            pltpu.VMEM((2, tok_rows, HEAD_DIM), fl),
            pltpu.VMEM((2, tok_rows, HEAD_DIM), fl),
            dma((NC, 2)), dma((NC, 3)), dma((NC, 3)), dma((NC, 2)), dma((NC, 2)),
            dma((NC, 3)), dma((NC, 3)), dma((NC, 4)), dma((NC, 4)),
            dma((NC,)), dma((NC,)), dma((NC,)), dma((NC,)), dma((NC,)),
            dma((1,)), dma((4,)), dma((4,)), dma((2 * TU,)), dma((TU,)), dma((TU,)), dma((TU,)),
            dma((NG, 2)), dma((NG, 2)), dma((NG,)), dma((2,)),
        ],
        compiler_params=pltpu.CompilerParams(
            collective_id=0, has_side_effects=True, vmem_limit_bytes=66_000_000),
    )(old_section_of, new_section_of, old_order.reshape(-1), new_order.reshape(-1),
      pieces, tokens, cos_in, sin_in)

    ids = jnp.arange(layers, dtype=jnp.int32)
    own = ids == jnp.sum(jnp.where(new_section_of == 2 * s + m % 2, ids, 0))
    crossed = jnp.sum(jnp.where(own, old_section_of, 0)) // 2 != s // 2
    key_first = jnp.sum(jnp.where(own, old_order[:, 0], 0)) == crossed.astype(jnp.int32)
    joined = jnp.concatenate(
        [jnp.where(key_first, kv[0], kv[1]), jnp.where(key_first, kv[1], kv[0])], axis=-1)
    return shards[None], joined[None]


def solution(mesh):
    in_specs = (P("section", None, "fsdp", None), P("section", "fsdp", None), P(), P(), P(), P())
    out_specs = (P("section", "fsdp", None), P("section", "fsdp", None))
    return jax.shard_map(
        per_device, mesh=mesh, in_specs=in_specs, out_specs=out_specs, check_vma=False
    )
```

```python
import math

import jax
import jax.numpy as jnp
from jax import lax
from jax.experimental import pallas as pl
from jax.experimental.pallas import tpu as pltpu
from jax.sharding import PartitionSpec as P

HEAD_DIM = 128
MESH = pl.DeviceIdType.MESH
NC = 8
NG = 4
TU = 8
XF = 1
SPLIT = 192


def body(oldsec, newsec, oldord, neword, freq, pieces, tokens, kv_out, shard_out, flag_out,
         pc, og, cand, tb, gb, wb, n2, sha, shb, xb, acc, ob, ct, st,
         pc_sem, rs, rr, zs, zr, xs, xr, ns, nr, shl, shs, shr,
         tl, tas, tar, ts, tr, tfs, tfr, osm, orm, olm):
    rows = pieces.shape[1]
    cw = pieces.shape[2] // NC
    gw = pieces.shape[2] // NG
    per = NC // NG
    tok_rows, width = tokens.shape
    layers = oldsec.shape[0]
    s = lax.axis_index("section")
    m = lax.axis_index("fsdp")
    y = s // 2
    c = s % 2
    j = m // 16
    x = (m // 4) % 4
    z = m % 4
    h = z % 2
    zh = z // 2
    prob = (j + zh) % 2
    is_a = c == prob
    is_b = c != prob
    alone = jnp.logical_and(c == j, zh == 0)
    not_alone = jnp.logical_or(c != j, zh != 0)

    def dev(yy, cc, jj, xx, zz):
        return (2 * yy + cc, jj * 16 + xx * 4 + zz)

    core_dev = dev(y, 1 - c, j, x, z)
    cross_dev = [dev(1 - y, k, 1 - j, x, z) for k in range(2)]
    zf = (z + 2) % 4
    xp, xm, xf = (x + 1) % 4, (x + 3) % 4, (x + 2) % 4
    xp_dev, xm_dev = (dev(y, c, j, xx, z) for xx in (xp, xm))

    def remote(src, dst, send, recv, device):
        return pltpu.make_async_remote_copy(
            src_ref=src, dst_ref=dst, send_sem=send, recv_sem=recv,
            device_id=device, device_id_type=MESH)

    def arrived(dst, send, recv, device):
        remote(dst, dst, send, recv, device).wait_recv()

    def pc_copy(i, a):
        return pltpu.make_async_copy(
            pieces.at[a, :, pl.ds(i * cw, cw)], pc.at[i, a], pc_sem.at[i, a])

    for i in range(NC):
        for a in range(2):
            pc_copy(i, a).start()

    def layer_of(section):
        found = jnp.int32(0)
        for l in range(layers):
            found = found + jnp.where(newsec[l] == section, l, 0)
        return found

    def entry(table, layer):
        found = jnp.int32(0)
        for l in range(layers):
            found = found + jnp.where(layer == l, table(l), 0)
        return found

    high = jnp.int32(0)
    for l in range(layers):
        high = jnp.where(oldsec[l] == s, l, high)
    row_high = entry(lambda l: newsec[l], high) // 2
    source = [entry(lambda l: oldsec[l], layer_of(2 * s + k)) for k in range(2)]
    gl = layer_of(2 * (2 * y + prob) + h)
    gl_crossed = jnp.where(entry(lambda l: oldsec[l], gl) // 2 == y, 0, 1)
    gl_old = entry(lambda l: oldord[0, l], gl)
    gl_new = entry(lambda l: neword[0, l], gl)
    gl_turn = (jnp.where(gl_old == gl_new, 0, 1) + gl_crossed + j + c) % 2
    is_key = gl_old == (c + gl_crossed) % 2
    ol = layer_of(2 * s + h)
    ol_crossed = jnp.where(entry(lambda l: oldsec[l], ol) // 2 == y, 0, 1)
    key_at = (entry(lambda l: oldord[0, l], ol) + ol_crossed) % 2
    flag_out[...] = jnp.zeros_like(flag_out) + key_at

    barrier = pltpu.get_barrier_semaphore()
    partners = cross_dev + [xp_dev, xm_dev]
    for n in range(1, 16):
        partners.append(dev(y, (c + n) % 2, (j + n // 2) % 2, x, (z + n // 4) % 4))
    for device in partners:
        pl.semaphore_signal(barrier, inc=1, device_id=device, device_id_type=MESH)
    pl.semaphore_wait(barrier, len(partners))

    tok_step = width // (2 * TU)
    quarter = width // 4

    def tok_send(v):
        u, a = v // 2, v % 2
        cols = pl.ds((a * TU + u) * tok_step, tok_step)
        parts = [(pl.ds(0, SPLIT), dev(y, a, 1 - j, x, z)),
                 (pl.ds(SPLIT, tok_rows - SPLIT), dev(y, a, j, x, zf))]
        return [remote(tokens.at[part, cols], xb.at[1, part, cols], ts.at[v, k], tr.at[u, k], device)
                for k, (part, device) in enumerate(parts)]

    def tok_here(u):
        cols = pl.ds(pl.multiple_of((c * TU + u) * tok_step, 128), tok_step)
        for k, part in enumerate((pl.ds(0, SPLIT), pl.ds(SPLIT, tok_rows - SPLIT))):
            arrived(xb.at[1, part, cols], tfs.at[u], tr.at[u, k], core_dev)

    def tok_pass(u):
        cols = pl.ds(pl.multiple_of((c * TU + u) * tok_step, 128), tok_step)
        return remote(xb.at[1, :, cols], xb.at[1, :, cols], tfs.at[u], tfr.at[u], core_dev)

    def tok_other(u):
        cols = pl.ds(pl.multiple_of(((1 - c) * TU + u) * tok_step, 128), tok_step)
        return remote(xb.at[1, :, cols], xb.at[1, :, cols], tfs.at[u], tfr.at[u], core_dev)

    def tok_core(k):
        cols = pl.ds(k * quarter, quarter)
        return remote(tokens.at[:, cols], xb.at[0, :, cols], tas.at[k], tar.at[k], core_dev)

    tok_local = pltpu.make_async_copy(tokens, xb.at[0], tl.at[0])
    tok_next = [0]

    def send_tokens(count):
        take = range(tok_next[0], min(tok_next[0] + count, 2 * TU))
        tok_next[0] += len(take)

        @pl.when(is_b)
        def _():
            for v in take:
                for copy in tok_send(v):
                    copy.start()

    def relay_copies(i):
        return [remote(og.at[i, k], cand.at[i, s], rs.at[i, k],
                       rr.at[i, 0] if k == 0 else rr.at[i, 1 + c], device)
                for k, device in enumerate([core_dev] + cross_dev)]

    relay_rows = [2 * y + 1 - c, 2 * (1 - y), 2 * (1 - y) + 1]

    def relay_send(i):
        for a in range(2):
            pc_copy(i, a).wait()

        def tile(t, carry):
            part = pl.ds(pl.multiple_of(t * 128, 128), 128)
            low_rows = pc[i, 0, part, :]
            high_rows = pc[i, 1, part, :]
            for k in range(3):
                og[i, k, part, :] = jnp.where(row_high == relay_rows[k], high_rows, low_rows)
            cand[i, s, part, :] = jnp.where(row_high == s, high_rows, low_rows)
            return carry

        lax.fori_loop(0, rows // 128, tile, 0)
        for copy in relay_copies(i):
            copy.start()

    slots = [x, xm, xp, xf]

    def place(slot, zz):
        return pl.ds(pl.multiple_of((slots[slot] * 4 + zz) * rows, rows), rows)

    def spread(i, slot):
        copies = []
        for k in range(2):
            src = gb.at[i, slots[slot], k] if i < XF else tb.at[i, k]
            target = 2 * ((c + j) % 2) + k
            for far in (1, 0):
                device = dev(y, j, (j + far) % 2, x, (target + 2 * far) % 4)
                copy = remote(src, wb.at[i, place(slot, z)], zs.at[i, slot, 2 * k + far],
                              zr.at[i, slot, z], device)
                here = jnp.logical_and(alone, h == k)
                copies.append((copy, None if far else jnp.logical_not(here)))
        return copies

    def spread_each(i, slot, act):
        for copy, needed in spread(i, slot):
            if needed is None:
                act(copy)
            else:
                @pl.when(needed)
                def _():
                    act(copy)

    def spread_start(i, slot):
        spread_each(i, slot, lambda copy: copy.start())

    def spread_arrived(i, slot):
        for n in range(1, 4):
            zz = (z + n) % 4
            arrived(wb.at[i, place(slot, zz)], zs.at[i, slot, 0], zr.at[i, slot, zz], core_dev)

        @pl.when(not_alone)
        def _():
            arrived(wb.at[i, place(slot, z)], zs.at[i, slot, 0], zr.at[i, slot, z], core_dev)

    def keep_first(i, slot):
        @pl.when(alone)
        def _():
            def tile(t, carry):
                part = pl.ds(pl.multiple_of(t * 128, 128), 128)
                to = pl.ds(pl.multiple_of((slots[slot] * 4 + z) * rows + t * 128, 128), 128)
                wb[i, to, :] = gb[i, slots[slot], h, part, :]
                return carry

            lax.fori_loop(0, rows // 128, tile, 0)

    def choose(i):
        arrived(cand.at[i, 2 * y + 1 - c], rs.at[i, 0], rr.at[i, 0], core_dev)
        for k in range(2):
            arrived(cand.at[i, 2 * (1 - y) + k], rs.at[i, 1 + k], rr.at[i, 1 + k], cross_dev[k])

        def tile(t, carry):
            part = pl.ds(pl.multiple_of(t * 128, 128), 128)
            four = [cand[i, k, part, :] for k in range(4)]
            for k in range(2):
                want = source[k]
                value = jnp.where(want < 2, jnp.where(want == 0, four[0], four[1]),
                                  jnp.where(want == 2, four[2], four[3]))
                if i < XF:
                    gb[i, x, k, part, :] = value
                else:
                    tb[i, k, part, :] = value
            return carry

        lax.fori_loop(0, rows // 128, tile, 0)
        if i < XF:
            for copy in first_own(i):
                copy.start()
        spread_start(i, 0)
        if i < XF:
            keep_first(i, 0)
        else:
            @pl.when(alone)
            def _():
                def keep(t, carry):
                    part = pl.ds(pl.multiple_of(t * 128, 128), 128)
                    to = pl.ds(pl.multiple_of((x * 4 + z) * rows + t * 128, 128), 128)
                    wb[i, to, :] = tb[i, h, part, :]
                    return carry

                lax.fori_loop(0, rows // 128, keep, 0)

    def first_own(i):
        mine = gb.at[i, x]
        return [remote(mine, mine, xs.at[i, 0], xr.at[i, 0], xp_dev),
                remote(mine, mine, xs.at[i, 1], xr.at[i, 1], xm_dev)]

    def first_pass_copies(i):
        left, right = gb.at[i, xm, 0], gb.at[i, xp, 1]
        return [remote(left, left, xs.at[i, 2], xr.at[i, 2], xp_dev),
                remote(right, right, xs.at[i, 3], xr.at[i, 3], xm_dev)]

    def first_pass(i):
        arrived(gb.at[i, xm], xs.at[i, 0], xr.at[i, 0], xp_dev)
        arrived(gb.at[i, xp], xs.at[i, 1], xr.at[i, 1], xm_dev)
        for copy in first_pass_copies(i):
            copy.start()
        for slot in (1, 2):
            spread_start(i, slot)
            keep_first(i, slot)

    def first_far(i):
        arrived(gb.at[i, xf, 0], xs.at[i, 2], xr.at[i, 2], xp_dev)
        arrived(gb.at[i, xf, 1], xs.at[i, 3], xr.at[i, 3], xm_dev)
        spread_start(i, 3)
        keep_first(i, 3)

    def block(i, xx, first, count):
        return wb.at[i, pl.ds(pl.multiple_of(xx * 4 * rows + first, rows), count)]

    def own_copies(i):
        mine = block(i, x, 0, 4 * rows)
        return [remote(mine, mine, xs.at[i, 0], xr.at[i, 0], xp_dev),
                remote(mine, mine, xs.at[i, 1], xr.at[i, 1], xm_dev)]

    def pass_copies(i):
        left = block(i, xm, 0, 2 * rows)
        right = block(i, xp, 2 * rows, 2 * rows)
        return [remote(left, left, xs.at[i, 2], xr.at[i, 2], xp_dev),
                remote(right, right, xs.at[i, 3], xr.at[i, 3], xm_dev)]

    pair = pl.ds(pl.multiple_of((x * 4 + z // 2 * 2) * rows, rows), 2 * rows)

    def near_copy(i):
        return remote(wb.at[i, pair], n2.at[i], ns.at[i], nr.at[i], core_dev)

    def x_own(i):
        spread_arrived(i, 0)
        if i >= XF:
            for copy in own_copies(i):
                copy.start()

        @pl.when(is_b)
        def _():
            near_copy(i).start()

    def x_pass(i):
        arrived(block(i, xm, 0, 4 * rows), xs.at[i, 0], xr.at[i, 0], xp_dev)
        first, second = pass_copies(i)
        first.start()
        arrived(block(i, xp, 0, 4 * rows), xs.at[i, 1], xr.at[i, 1], xm_dev)
        second.start()

    def far_arrived(i):
        if i < XF:
            for slot in (1, 2, 3):
                spread_arrived(i, slot)
            return
        arrived(block(i, xf, 0, 2 * rows), xs.at[i, 2], xr.at[i, 2], xp_dev)
        arrived(block(i, xf, 2 * rows, 2 * rows), xs.at[i, 3], xr.at[i, 3], xm_dev)

    def shard_local(i):
        return pltpu.make_async_copy(sha.at[i], shard_out.at[:, pl.ds(i * cw, cw)], shl.at[i])

    def shard_far(i):
        return remote(shb.at[i], shard_out.at[:, pl.ds(i * cw, cw)], shs.at[i], shr.at[i],
                      dev(y, c, 1 - j, x, z))

    def shard(i):
        @pl.when(is_a)
        def _():
            near_copy(i).wait_recv()

            def tile(t, carry):
                part = pl.ds(pl.multiple_of(t * 128, 128), 128)
                near = pl.ds(pl.multiple_of((x * 4 + z // 2 * 2) * rows + t * 128, 128), 128)
                mine = wb[i, near, :]
                other = n2[i, part, :]
                sha[i, part, :] = jnp.where(gl_turn == 0, mine, other)
                shb[i, part, :] = jnp.where(gl_turn == 0, other, mine)
                return carry

            lax.fori_loop(0, 2 * rows // 128, tile, 0)

    def shard_send(i):
        @pl.when(is_a)
        def _():
            shard_local(i).start()
            shard_far(i).start()

    def multiply(g, xx, half):
        first = pl.multiple_of(xx * 4 * rows + half * 2 * rows, 2 * rows)
        ks = pl.ds(first, 2 * rows)
        weight = jnp.concatenate([wb[per * g + k, ks, :] for k in range(per)], axis=1)
        for slot in range(2):
            acc[slot] += jnp.dot(xb[slot, :, ks], weight, preferred_element_type=jnp.float32)

    def finish(g):
        def tile(t, carry):
            part = pl.ds(pl.multiple_of(t * 64, 64), 64)
            for slot in range(2):
                cosine = ct[slot, part, :]
                sine = st[slot, part, :]
                for head in range(gw // HEAD_DIM):
                    cols = slice(head * HEAD_DIM, (head + 1) * HEAD_DIM)
                    value = acc[slot, part, cols]
                    turned = value * cosine + pltpu.roll(value, HEAD_DIM // 2, 1) * sine
                    ob[g, slot, part, cols] = turned.astype(jnp.bfloat16)
            return carry

        lax.fori_loop(0, tok_rows // 64, tile, 0)

    def out_local(g):
        return pltpu.make_async_copy(
            ob.at[g, 0], kv_out.at[c, :, pl.ds(g * gw, gw)], olm.at[g])

    def out_near(g):
        return remote(ob.at[g, 0], kv_out.at[c, :, pl.ds(g * gw, gw)],
                      osm.at[g, 0], orm.at[g, c], core_dev)

    def out_parts(g, q):
        cols = pl.ds(g * gw, gw)
        return [kv_out.at[q, pl.ds(0, SPLIT), cols],
                kv_out.at[q, pl.ds(SPLIT, tok_rows - SPLIT), cols]]

    def out_far(g):
        to_y, to_z = out_parts(g, c)
        return [remote(ob.at[g, 1, pl.ds(0, SPLIT)], to_y, osm.at[g, 1], orm.at[g, c],
                       dev(y, prob, 1 - j, x, z)),
                remote(ob.at[g, 1, pl.ds(SPLIT, tok_rows - SPLIT)], to_z, osm.at[g, 2],
                       orm.at[g, 2 + c], dev(y, prob, j, x, zf))]

    def out_send(g):
        for copy in out_far(g):
            copy.start()

        @pl.when(is_a)
        def _():
            out_local(g).start()

        @pl.when(is_b)
        def _():
            out_near(g).start()

    def tables():
        first = m // 2 * tok_rows
        by_y = (m // 2 + 8) % 16 * tok_rows
        by_z = (m // 2 + 1 - 2 * zh) * tok_rows
        lane = lax.broadcasted_iota(jnp.int32, (64, HEAD_DIM), 1)
        row = lax.broadcasted_iota(jnp.int32, (64, HEAD_DIM), 0)

        def tile(t, carry):
            part = pl.ds(pl.multiple_of(t * 64, 64), 64)
            for slot in range(2):
                base = first if slot == 0 else jnp.where(t * 64 < SPLIT, by_y, by_z)
                position = (base + t * 64 + row).astype(jnp.float32)
                angle = position * freq[0:1, :]
                sine = jnp.sin(angle)
                sine = jnp.where(lane < HEAD_DIM // 2, -sine, sine)
                ct[slot, part, :] = jnp.where(is_key, jnp.cos(angle), 1.0)
                st[slot, part, :] = jnp.where(is_key, sine, 0.0)
            return carry

        lax.fori_loop(0, tok_rows // 64, tile, 0)

    send_tokens(2)
    for i in range(NC):
        relay_send(i)
    for t in range(NC + 1):
        if t < NC:
            choose(t)
            if t >= 1:
                send_tokens(2)
        if t == 0:
            @pl.when(is_a)
            def _():
                tok_local.start()
                for k in range(4):
                    tok_core(k).start()
        if 0 < t <= XF:
            first_pass(t - 1)
        if t >= 1 and t - 1 >= XF:
            x_own(t - 1)
        if 2 <= t < 2 + XF:
            first_far(t - 2)
            x_own(t - 2)
    send_tokens(2 * TU)
    tables()
    for i in range(NC):
        if i >= XF:
            x_pass(i)
        shard(i)
        if i >= 2:
            tok_here(i - 2)
            tok_pass(i - 2).start()
    for u in range(NC - 2, TU):
        tok_here(u)
        tok_pass(u).start()
    for i in range(NC):
        shard_send(i)

    @pl.when(is_a)
    def _():
        tok_local.wait()

    @pl.when(is_b)
    def _():
        for k in range(4):
            tok_core(k).wait_recv()

    for u in range(TU):
        tok_other(u).wait_recv()

    for g in range(NG):
        acc[...] = jnp.zeros_like(acc)

        def near_block(t, carry):
            b = t // 2
            multiply(g, (x + b + b // 2) % 4, t % 2)
            return carry

        for k in range(per):
            if per * g + k < XF:
                far_arrived(per * g + k)
        lax.fori_loop(0, 6, near_block, 0)
        for k in range(per):
            if per * g + k >= XF:
                far_arrived(per * g + k)

        def far_block(t, carry):
            multiply(g, xf, t)
            return carry

        lax.fori_loop(0, 2, far_block, 0)
        finish(g)
        out_send(g)

    for i in range(NC):
        for copy in relay_copies(i):
            copy.wait_send()
        for copy in (first_own(i) + first_pass_copies(i) if i < XF else own_copies(i) + pass_copies(i)):
            copy.wait_send()
        for slot in range(4 if i < XF else 1):
            spread_each(i, slot, lambda copy: copy.wait_send())

    @pl.when(is_a)
    def _():
        for k in range(4):
            tok_core(k).wait_send()
        for i in range(NC):
            shard_local(i).wait()
            shard_far(i).wait_send()
        for g in range(NG):
            out_local(g).wait()
            arrived(kv_out.at[1 - c, :, pl.ds(g * gw, gw)], osm.at[g, 0], orm.at[g, 1 - c], core_dev)

    @pl.when(is_b)
    def _():
        for v in range(2 * TU):
            for copy in tok_send(v):
                copy.wait_send()
        for i in range(NC):
            near_copy(i).wait_send()
            shard_far(i).wait_recv()
        for g in range(NG):
            out_near(g).wait_send()
            for q in range(2):
                for k, part in enumerate(out_parts(g, q)):
                    arrived(part, osm.at[g, 0], orm.at[g, 2 * k + q], core_dev)

    for u in range(TU):
        tok_pass(u).wait_send()
    for g in range(NG):
        for copy in out_far(g):
            copy.wait_send()


def per_device(old_pieces, section_inputs, old_section_of, new_section_of, old_order, new_order):
    pieces = old_pieces[0]
    tokens = section_inputs[0]
    _, rows, kv_width = pieces.shape
    tok_rows, width = tokens.shape
    cw, gw = kv_width // NC, kv_width // NG

    half_dim = HEAD_DIM // 2
    freq_index = (jnp.arange(HEAD_DIM, dtype=jnp.int32) % half_dim).astype(jnp.float32)
    inverse_freq = jnp.exp(freq_index * (-2.0 * math.log(500000.0) / HEAD_DIM))
    freq = jnp.broadcast_to(inverse_freq[None, :], (8, HEAD_DIM))

    dma = pltpu.SemaphoreType.DMA
    bf, fl = jnp.bfloat16, jnp.float32
    hbm = pl.BlockSpec(memory_space=pltpu.HBM)
    vmem = pl.BlockSpec(memory_space=pltpu.VMEM)
    smem = pl.BlockSpec(memory_space=pltpu.SMEM)
    kv, shards, flag = pl.pallas_call(
        body,
        out_shape=(jax.ShapeDtypeStruct((2, tok_rows, kv_width), bf),
                   jax.ShapeDtypeStruct((2 * rows, kv_width), bf),
                   jax.ShapeDtypeStruct((8, 128), jnp.int32)),
        in_specs=[smem] * 4 + [vmem] + [hbm] * 2,
        out_specs=(hbm, hbm, vmem),
        scratch_shapes=[
            pltpu.VMEM((NC, 2, rows, cw), bf),
            pltpu.VMEM((NC, 3, rows, cw), bf),
            pltpu.VMEM((NC, 4, rows, cw), bf),
            pltpu.VMEM((NC, 2, rows, cw), bf),
            pltpu.VMEM((max(XF, 1), 4, 2, rows, cw), bf),
            pltpu.VMEM((NC, width, cw), bf),
            pltpu.VMEM((NC, 2 * rows, cw), bf),
            pltpu.VMEM((NC, 2 * rows, cw), bf),
            pltpu.VMEM((NC, 2 * rows, cw), bf),
            pltpu.VMEM((2, tok_rows, width), bf),
            pltpu.VMEM((2, tok_rows, gw), fl),
            pltpu.VMEM((NG, 2, tok_rows, gw), bf),
            pltpu.VMEM((2, tok_rows, HEAD_DIM), fl),
            pltpu.VMEM((2, tok_rows, HEAD_DIM), fl),
            dma((NC, 2)), dma((NC, 3)), dma((NC, 3)),
            dma((NC, 4, 4)), dma((NC, 4, 4)), dma((NC, 4)), dma((NC, 4)),
            dma((NC,)), dma((NC,)), dma((NC,)), dma((NC,)), dma((NC,)),
            dma((1,)), dma((4,)), dma((4,)), dma((2 * TU, 2)), dma((TU, 2)), dma((TU,)), dma((TU,)),
            dma((NG, 3)), dma((NG, 4)), dma((NG,)),
        ],
        compiler_params=pltpu.CompilerParams(
            collective_id=0, has_side_effects=True, vmem_limit_bytes=66_000_000),
    )(old_section_of, new_section_of, old_order.T, new_order.T, freq, pieces, tokens)

    swapped = flag[0, 0] == 1
    joined = jnp.where(swapped, jnp.concatenate([kv[1], kv[0]], axis=-1),
                       jnp.concatenate([kv[0], kv[1]], axis=-1))
    return shards[None], joined[None]


def solution(mesh):
    in_specs = (P("section", None, "fsdp", None), P("section", "fsdp", None), P(), P(), P(), P())
    out_specs = (P("section", "fsdp", None), P("section", "fsdp", None))
    return jax.shard_map(
        per_device, mesh=mesh, in_specs=in_specs, out_specs=out_specs, check_vma=False
    )
```

```python
import math

import jax
import jax.numpy as jnp
from jax import lax
from jax.experimental import pallas as pl
from jax.experimental.pallas import tpu as pltpu
from jax.sharding import PartitionSpec as P

HEAD_DIM = 128
MESH = pl.DeviceIdType.MESH
NC = 8
NG = 4
TU = 8
XF = 1
SPLIT = 192


def body(oldsec, newsec, oldord, neword, freq, pieces, tokens, kv_out, shard_out, flag_out,
         pc, og, cand, tb, gb, wb, n2, sha, shb, xb, acc, ob, ct, st,
         pc_sem, rs, rr, zs, zr, xs, xr, ns, nr, shl, shs, shr,
         tl, tas, tar, ts, tr, tfs, tfr, osm, orm, olm):
    rows = pieces.shape[1]
    cw = pieces.shape[2] // NC
    gw = pieces.shape[2] // NG
    per = NC // NG
    tok_rows, width = tokens.shape
    layers = oldsec.shape[0]
    s = lax.axis_index("section")
    m = lax.axis_index("fsdp")
    y = s // 2
    c = s % 2
    j = m // 16
    x = (m // 4) % 4
    z = m % 4
    h = z % 2
    zh = z // 2
    prob = (j + zh) % 2
    is_a = c == prob
    is_b = c != prob
    alone = jnp.logical_and(c == j, zh == 0)
    not_alone = jnp.logical_or(c != j, zh != 0)

    def dev(yy, cc, jj, xx, zz):
        return (2 * yy + cc, jj * 16 + xx * 4 + zz)

    core_dev = dev(y, 1 - c, j, x, z)
    cross_dev = [dev(1 - y, k, 1 - j, x, z) for k in range(2)]
    zf = (z + 2) % 4
    xp, xm, xf = (x + 1) % 4, (x + 3) % 4, (x + 2) % 4
    xp_dev, xm_dev = (dev(y, c, j, xx, z) for xx in (xp, xm))

    def remote(src, dst, send, recv, device):
        return pltpu.make_async_remote_copy(
            src_ref=src, dst_ref=dst, send_sem=send, recv_sem=recv,
            device_id=device, device_id_type=MESH)

    def arrived(dst, send, recv, device):
        remote(dst, dst, send, recv, device).wait_recv()

    def pc_copy(i, a):
        return pltpu.make_async_copy(
            pieces.at[a, :, pl.ds(i * cw, cw)], pc.at[i, a], pc_sem.at[i, a])

    for i in range(NC):
        for a in range(2):
            pc_copy(i, a).start()

    def layer_of(section):
        found = jnp.int32(0)
        for l in range(layers):
            found = found + jnp.where(newsec[l] == section, l, 0)
        return found

    def entry(table, layer):
        found = jnp.int32(0)
        for l in range(layers):
            found = found + jnp.where(layer == l, table(l), 0)
        return found

    high = jnp.int32(0)
    for l in range(layers):
        high = jnp.where(oldsec[l] == s, l, high)
    row_high = entry(lambda l: newsec[l], high) // 2
    source = [entry(lambda l: oldsec[l], layer_of(2 * s + k)) for k in range(2)]
    gl = layer_of(2 * (2 * y + prob) + h)
    gl_crossed = jnp.where(entry(lambda l: oldsec[l], gl) // 2 == y, 0, 1)
    gl_old = entry(lambda l: oldord[0, l], gl)
    gl_new = entry(lambda l: neword[0, l], gl)
    gl_turn = (jnp.where(gl_old == gl_new, 0, 1) + gl_crossed + j + c) % 2
    is_key = gl_old == (c + gl_crossed) % 2
    ol = layer_of(2 * s + h)
    ol_crossed = jnp.where(entry(lambda l: oldsec[l], ol) // 2 == y, 0, 1)
    key_at = (entry(lambda l: oldord[0, l], ol) + ol_crossed) % 2
    flag_out[...] = jnp.zeros_like(flag_out) + key_at

    barrier = pltpu.get_barrier_semaphore()
    partners = cross_dev + [xp_dev, xm_dev]
    for n in range(1, 16):
        partners.append(dev(y, (c + n) % 2, (j + n // 2) % 2, x, (z + n // 4) % 4))
    for device in partners:
        pl.semaphore_signal(barrier, inc=1, device_id=device, device_id_type=MESH)
    pl.semaphore_wait(barrier, len(partners))

    tok_step = width // (2 * TU)
    quarter = width // 4

    def tok_send(v):
        u, a = v // 2, v % 2
        cols = pl.ds((a * TU + u) * tok_step, tok_step)
        parts = [(pl.ds(0, SPLIT), dev(y, a, 1 - j, x, z)),
                 (pl.ds(SPLIT, tok_rows - SPLIT), dev(y, a, j, x, zf))]
        return [remote(tokens.at[part, cols], xb.at[1, part, cols], ts.at[v, k], tr.at[u, k], device)
                for k, (part, device) in enumerate(parts)]

    def tok_here(u):
        cols = pl.ds(pl.multiple_of((c * TU + u) * tok_step, 128), tok_step)
        for k, part in enumerate((pl.ds(0, SPLIT), pl.ds(SPLIT, tok_rows - SPLIT))):
            arrived(xb.at[1, part, cols], tfs.at[u], tr.at[u, k], core_dev)

    def tok_pass(u):
        cols = pl.ds(pl.multiple_of((c * TU + u) * tok_step, 128), tok_step)
        return remote(xb.at[1, :, cols], xb.at[1, :, cols], tfs.at[u], tfr.at[u], core_dev)

    def tok_other(u):
        cols = pl.ds(pl.multiple_of(((1 - c) * TU + u) * tok_step, 128), tok_step)
        return remote(xb.at[1, :, cols], xb.at[1, :, cols], tfs.at[u], tfr.at[u], core_dev)

    def tok_core(k):
        cols = pl.ds(k * quarter, quarter)
        return remote(tokens.at[:, cols], xb.at[0, :, cols], tas.at[k], tar.at[k], core_dev)

    tok_local = pltpu.make_async_copy(tokens, xb.at[0], tl.at[0])
    tok_next = [0]

    def send_tokens(count):
        take = range(tok_next[0], min(tok_next[0] + count, 2 * TU))
        tok_next[0] += len(take)

        @pl.when(is_b)
        def _():
            for v in take:
                for copy in tok_send(v):
                    copy.start()

    def relay_copies(i):
        return [remote(og.at[i, k], cand.at[i, s], rs.at[i, k],
                       rr.at[i, 0] if k == 0 else rr.at[i, 1 + c], device)
                for k, device in enumerate([core_dev] + cross_dev)]

    relay_rows = [2 * y + 1 - c, 2 * (1 - y), 2 * (1 - y) + 1]

    def relay_send(i):
        for a in range(2):
            pc_copy(i, a).wait()

        def tile(t, carry):
            part = pl.ds(pl.multiple_of(t * 128, 128), 128)
            low_rows = pc[i, 0, part, :]
            high_rows = pc[i, 1, part, :]
            for k in range(3):
                og[i, k, part, :] = jnp.where(row_high == relay_rows[k], high_rows, low_rows)
            cand[i, s, part, :] = jnp.where(row_high == s, high_rows, low_rows)
            return carry

        lax.fori_loop(0, rows // 128, tile, 0)
        for copy in relay_copies(i):
            copy.start()

    slots = [x, xm, xp, xf]

    def place(slot, zz):
        return pl.ds(pl.multiple_of((slots[slot] * 4 + zz) * rows, rows), rows)

    def spread(i, slot):
        copies = []
        for k in range(2):
            src = gb.at[i, slots[slot], k] if i < XF else tb.at[i, k]
            target = 2 * ((c + j) % 2) + k
            for far in (1, 0):
                device = dev(y, j, (j + far) % 2, x, (target + 2 * far) % 4)
                copy = remote(src, wb.at[i, place(slot, z)], zs.at[i, slot, 2 * k + far],
                              zr.at[i, slot, z], device)
                here = jnp.logical_and(alone, h == k)
                copies.append((copy, None if far else jnp.logical_not(here)))
        return copies

    def spread_each(i, slot, act):
        for copy, needed in spread(i, slot):
            if needed is None:
                act(copy)
            else:
                @pl.when(needed)
                def _():
                    act(copy)

    def spread_start(i, slot):
        spread_each(i, slot, lambda copy: copy.start())

    def spread_arrived(i, slot):
        for n in range(1, 4):
            zz = (z + n) % 4
            arrived(wb.at[i, place(slot, zz)], zs.at[i, slot, 0], zr.at[i, slot, zz], core_dev)

        @pl.when(not_alone)
        def _():
            arrived(wb.at[i, place(slot, z)], zs.at[i, slot, 0], zr.at[i, slot, z], core_dev)

    def keep_first(i, slot):
        @pl.when(alone)
        def _():
            def tile(t, carry):
                part = pl.ds(pl.multiple_of(t * 128, 128), 128)
                to = pl.ds(pl.multiple_of((slots[slot] * 4 + z) * rows + t * 128, 128), 128)
                wb[i, to, :] = gb[i, slots[slot], h, part, :]
                return carry

            lax.fori_loop(0, rows // 128, tile, 0)

    def choose(i):
        arrived(cand.at[i, 2 * y + 1 - c], rs.at[i, 0], rr.at[i, 0], core_dev)
        for k in range(2):
            arrived(cand.at[i, 2 * (1 - y) + k], rs.at[i, 1 + k], rr.at[i, 1 + k], cross_dev[k])

        def tile(t, carry):
            part = pl.ds(pl.multiple_of(t * 128, 128), 128)
            four = [cand[i, k, part, :] for k in range(4)]
            for k in range(2):
                want = source[k]
                value = jnp.where(want < 2, jnp.where(want == 0, four[0], four[1]),
                                  jnp.where(want == 2, four[2], four[3]))
                if i < XF:
                    gb[i, x, k, part, :] = value
                else:
                    tb[i, k, part, :] = value
            return carry

        lax.fori_loop(0, rows // 128, tile, 0)
        if i < XF:
            for copy in first_own(i):
                copy.start()
        spread_start(i, 0)
        if i < XF:
            keep_first(i, 0)
        else:
            @pl.when(alone)
            def _():
                def keep(t, carry):
                    part = pl.ds(pl.multiple_of(t * 128, 128), 128)
                    to = pl.ds(pl.multiple_of((x * 4 + z) * rows + t * 128, 128), 128)
                    wb[i, to, :] = tb[i, h, part, :]
                    return carry

                lax.fori_loop(0, rows // 128, keep, 0)

    def first_own(i):
        mine = gb.at[i, x]
        return [remote(mine, mine, xs.at[i, 0], xr.at[i, 0], xp_dev),
                remote(mine, mine, xs.at[i, 1], xr.at[i, 1], xm_dev)]

    def first_pass_copies(i):
        left, right = gb.at[i, xm, 0], gb.at[i, xp, 1]
        return [remote(left, left, xs.at[i, 2], xr.at[i, 2], xp_dev),
                remote(right, right, xs.at[i, 3], xr.at[i, 3], xm_dev)]

    def first_pass(i):
        arrived(gb.at[i, xm], xs.at[i, 0], xr.at[i, 0], xp_dev)
        arrived(gb.at[i, xp], xs.at[i, 1], xr.at[i, 1], xm_dev)
        for copy in first_pass_copies(i):
            copy.start()

    def first_far(i):
        arrived(gb.at[i, xf, 0], xs.at[i, 2], xr.at[i, 2], xp_dev)
        arrived(gb.at[i, xf, 1], xs.at[i, 3], xr.at[i, 3], xm_dev)
        for slot in (1, 2, 3):
            spread_start(i, slot)
            keep_first(i, slot)

    def block(i, xx, first, count):
        return wb.at[i, pl.ds(pl.multiple_of(xx * 4 * rows + first, rows), count)]

    def own_copies(i):
        mine = block(i, x, 0, 4 * rows)
        return [remote(mine, mine, xs.at[i, 0], xr.at[i, 0], xp_dev),
                remote(mine, mine, xs.at[i, 1], xr.at[i, 1], xm_dev)]

    def pass_copies(i):
        left = block(i, xm, 0, 2 * rows)
        right = block(i, xp, 2 * rows, 2 * rows)
        return [remote(left, left, xs.at[i, 2], xr.at[i, 2], xp_dev),
                remote(right, right, xs.at[i, 3], xr.at[i, 3], xm_dev)]

    pair = pl.ds(pl.multiple_of((x * 4 + z // 2 * 2) * rows, rows), 2 * rows)

    def near_copy(i):
        return remote(wb.at[i, pair], n2.at[i], ns.at[i], nr.at[i], core_dev)

    def x_own(i):
        spread_arrived(i, 0)
        if i >= XF:
            for copy in own_copies(i):
                copy.start()

        @pl.when(is_b)
        def _():
            near_copy(i).start()

    def x_pass(i):
        arrived(block(i, xm, 0, 4 * rows), xs.at[i, 0], xr.at[i, 0], xp_dev)
        first, second = pass_copies(i)
        first.start()
        arrived(block(i, xp, 0, 4 * rows), xs.at[i, 1], xr.at[i, 1], xm_dev)
        second.start()

    def far_arrived(i):
        if i < XF:
            for slot in (1, 2, 3):
                spread_arrived(i, slot)
            return
        arrived(block(i, xf, 0, 2 * rows), xs.at[i, 2], xr.at[i, 2], xp_dev)
        arrived(block(i, xf, 2 * rows, 2 * rows), xs.at[i, 3], xr.at[i, 3], xm_dev)

    def shard_local(i):
        return pltpu.make_async_copy(sha.at[i], shard_out.at[:, pl.ds(i * cw, cw)], shl.at[i])

    def shard_far(i):
        return remote(shb.at[i], shard_out.at[:, pl.ds(i * cw, cw)], shs.at[i], shr.at[i],
                      dev(y, c, 1 - j, x, z))

    def shard(i):
        @pl.when(is_a)
        def _():
            near_copy(i).wait_recv()

            def tile(t, carry):
                part = pl.ds(pl.multiple_of(t * 128, 128), 128)
                near = pl.ds(pl.multiple_of((x * 4 + z // 2 * 2) * rows + t * 128, 128), 128)
                mine = wb[i, near, :]
                other = n2[i, part, :]
                sha[i, part, :] = jnp.where(gl_turn == 0, mine, other)
                shb[i, part, :] = jnp.where(gl_turn == 0, other, mine)
                return carry

            lax.fori_loop(0, 2 * rows // 128, tile, 0)

    def shard_send(i):
        @pl.when(is_a)
        def _():
            shard_local(i).start()
            shard_far(i).start()

    def multiply(g, slots_now, xx, half):
        first = pl.multiple_of(xx * 4 * rows + half * 2 * rows, 2 * rows)
        ks = pl.ds(first, 2 * rows)
        weight = jnp.concatenate([wb[per * g + k, ks, :] for k in range(per)], axis=1)
        for slot in slots_now:
            acc[g, slot] += jnp.dot(xb[slot, :, ks], weight, preferred_element_type=jnp.float32)

    def near(g, slots_now):
        for slot in slots_now:
            acc[g, slot] = jnp.zeros(acc.shape[2:], acc.dtype)

        def near_block(t, carry):
            b = t // 2
            multiply(g, slots_now, (x + b + b // 2) % 4, t % 2)
            return carry

        lax.fori_loop(0, 6, near_block, 0)

    def far(g):
        def far_block(t, carry):
            multiply(g, (0, 1), xf, t)
            return carry

        lax.fori_loop(0, 2, far_block, 0)

    def finish(g):
        def tile(t, carry):
            part = pl.ds(pl.multiple_of(t * 64, 64), 64)
            for slot in range(2):
                cosine = ct[slot, part, :]
                sine = st[slot, part, :]
                for head in range(gw // HEAD_DIM):
                    cols = slice(head * HEAD_DIM, (head + 1) * HEAD_DIM)
                    value = acc[g, slot, part, cols]
                    turned = value * cosine + pltpu.roll(value, HEAD_DIM // 2, 1) * sine
                    ob[g, slot, part, cols] = turned.astype(jnp.bfloat16)
            return carry

        lax.fori_loop(0, tok_rows // 64, tile, 0)

    def out_local(g):
        return pltpu.make_async_copy(
            ob.at[g, 0], kv_out.at[c, :, pl.ds(g * gw, gw)], olm.at[g])

    def out_near(g):
        return remote(ob.at[g, 0], kv_out.at[c, :, pl.ds(g * gw, gw)],
                      osm.at[g, 0], orm.at[g, c], core_dev)

    def out_parts(g, q):
        cols = pl.ds(g * gw, gw)
        return [kv_out.at[q, pl.ds(0, SPLIT), cols],
                kv_out.at[q, pl.ds(SPLIT, tok_rows - SPLIT), cols]]

    def out_far(g):
        to_y, to_z = out_parts(g, c)
        return [remote(ob.at[g, 1, pl.ds(0, SPLIT)], to_y, osm.at[g, 1], orm.at[g, c],
                       dev(y, prob, 1 - j, x, z)),
                remote(ob.at[g, 1, pl.ds(SPLIT, tok_rows - SPLIT)], to_z, osm.at[g, 2],
                       orm.at[g, 2 + c], dev(y, prob, j, x, zf))]

    def out_send(g):
        for copy in out_far(g):
            copy.start()

        @pl.when(is_a)
        def _():
            out_local(g).start()

        @pl.when(is_b)
        def _():
            out_near(g).start()

    def tables():
        first = m // 2 * tok_rows
        by_y = (m // 2 + 8) % 16 * tok_rows
        by_z = (m // 2 + 1 - 2 * zh) * tok_rows
        lane = lax.broadcasted_iota(jnp.int32, (64, HEAD_DIM), 1)
        row = lax.broadcasted_iota(jnp.int32, (64, HEAD_DIM), 0)

        def tile(t, carry):
            part = pl.ds(pl.multiple_of(t * 64, 64), 64)
            for slot in range(2):
                base = first if slot == 0 else jnp.where(t * 64 < SPLIT, by_y, by_z)
                position = (base + t * 64 + row).astype(jnp.float32)
                angle = position * freq[0:1, :]
                sine = jnp.sin(angle)
                sine = jnp.where(lane < HEAD_DIM // 2, -sine, sine)
                ct[slot, part, :] = jnp.where(is_key, jnp.cos(angle), 1.0)
                st[slot, part, :] = jnp.where(is_key, sine, 0.0)
            return carry

        lax.fori_loop(0, tok_rows // 64, tile, 0)

    def token_pass(u):
        tok_here(u)
        tok_pass(u).start()

    send_tokens(2)
    for i in range(NC):
        relay_send(i)
    choose(0)

    @pl.when(is_a)
    def _():
        tok_local.start()
        for k in range(4):
            tok_core(k).start()

    choose(1)
    first_pass(0)
    choose(2)
    x_own(1)
    choose(3)
    x_own(2)
    choose(4)
    x_own(3)
    choose(5)
    x_own(4)
    x_pass(1)
    choose(6)
    x_own(5)
    choose(7)
    send_tokens(2 * TU)
    x_own(6)
    x_pass(2)
    x_own(7)
    tables()
    x_own(0)

    @pl.when(is_a)
    def _():
        tok_local.wait()

    @pl.when(is_b)
    def _():
        for k in range(4):
            tok_core(k).wait_recv()

    x_pass(3)
    for i in range(0, 4):
        shard(i)
        shard_send(i)
    near(1, (0,))
    token_pass(0)
    token_pass(1)
    x_pass(4)
    token_pass(2)
    token_pass(3)
    x_pass(5)
    first_far(0)
    for i in range(4, 8):
        shard(i)
        shard_send(i)
    near(2, (0,))
    token_pass(4)
    x_pass(6)
    token_pass(5)
    token_pass(6)
    token_pass(7)
    x_pass(7)
    near(3, (0,))
    for u in range(TU):
        tok_other(u).wait_recv()
    for g in (1, 2, 3):
        near(g, (1,))
    for g in (1, 2, 0, 3):
        for k in range(per):
            far_arrived(per * g + k)
        if g == 0:
            near(g, (0, 1))
        far(g)
        finish(g)
        out_send(g)

    for i in range(NC):
        for copy in relay_copies(i):
            copy.wait_send()
        for copy in (first_own(i) + first_pass_copies(i) if i < XF else own_copies(i) + pass_copies(i)):
            copy.wait_send()
        for slot in range(4 if i < XF else 1):
            spread_each(i, slot, lambda copy: copy.wait_send())

    @pl.when(is_a)
    def _():
        for k in range(4):
            tok_core(k).wait_send()
        for i in range(NC):
            shard_local(i).wait()
            shard_far(i).wait_send()
        for g in range(NG):
            out_local(g).wait()
            arrived(kv_out.at[1 - c, :, pl.ds(g * gw, gw)], osm.at[g, 0], orm.at[g, 1 - c], core_dev)

    @pl.when(is_b)
    def _():
        for v in range(2 * TU):
            for copy in tok_send(v):
                copy.wait_send()
        for i in range(NC):
            near_copy(i).wait_send()
            shard_far(i).wait_recv()
        for g in range(NG):
            out_near(g).wait_send()
            for q in range(2):
                for k, part in enumerate(out_parts(g, q)):
                    arrived(part, osm.at[g, 0], orm.at[g, 2 * k + q], core_dev)

    for u in range(TU):
        tok_pass(u).wait_send()
    for g in range(NG):
        for copy in out_far(g):
            copy.wait_send()


def per_device(old_pieces, section_inputs, old_section_of, new_section_of, old_order, new_order):
    pieces = old_pieces[0]
    tokens = section_inputs[0]
    _, rows, kv_width = pieces.shape
    tok_rows, width = tokens.shape
    cw, gw = kv_width // NC, kv_width // NG

    half_dim = HEAD_DIM // 2
    freq_index = (jnp.arange(HEAD_DIM, dtype=jnp.int32) % half_dim).astype(jnp.float32)
    inverse_freq = jnp.exp(freq_index * (-2.0 * math.log(500000.0) / HEAD_DIM))
    freq = jnp.broadcast_to(inverse_freq[None, :], (8, HEAD_DIM))

    dma = pltpu.SemaphoreType.DMA
    bf, fl = jnp.bfloat16, jnp.float32
    hbm = pl.BlockSpec(memory_space=pltpu.HBM)
    vmem = pl.BlockSpec(memory_space=pltpu.VMEM)
    smem = pl.BlockSpec(memory_space=pltpu.SMEM)
    kv, shards, flag = pl.pallas_call(
        body,
        out_shape=(jax.ShapeDtypeStruct((2, tok_rows, kv_width), bf),
                   jax.ShapeDtypeStruct((2 * rows, kv_width), bf),
                   jax.ShapeDtypeStruct((8, 128), jnp.int32)),
        in_specs=[smem] * 4 + [vmem] + [hbm] * 2,
        out_specs=(hbm, hbm, vmem),
        scratch_shapes=[
            pltpu.VMEM((NC, 2, rows, cw), bf),
            pltpu.VMEM((NC, 3, rows, cw), bf),
            pltpu.VMEM((NC, 4, rows, cw), bf),
            pltpu.VMEM((NC, 2, rows, cw), bf),
            pltpu.VMEM((max(XF, 1), 4, 2, rows, cw), bf),
            pltpu.VMEM((NC, width, cw), bf),
            pltpu.VMEM((NC, 2 * rows, cw), bf),
            pltpu.VMEM((NC, 2 * rows, cw), bf),
            pltpu.VMEM((NC, 2 * rows, cw), bf),
            pltpu.VMEM((2, tok_rows, width), bf),
            pltpu.VMEM((NG, 2, tok_rows, gw), fl),
            pltpu.VMEM((NG, 2, tok_rows, gw), bf),
            pltpu.VMEM((2, tok_rows, HEAD_DIM), fl),
            pltpu.VMEM((2, tok_rows, HEAD_DIM), fl),
            dma((NC, 2)), dma((NC, 3)), dma((NC, 3)),
            dma((NC, 4, 4)), dma((NC, 4, 4)), dma((NC, 4)), dma((NC, 4)),
            dma((NC,)), dma((NC,)), dma((NC,)), dma((NC,)), dma((NC,)),
            dma((1,)), dma((4,)), dma((4,)), dma((2 * TU, 2)), dma((TU, 2)), dma((TU,)), dma((TU,)),
            dma((NG, 3)), dma((NG, 4)), dma((NG,)),
        ],
        compiler_params=pltpu.CompilerParams(
            collective_id=0, has_side_effects=True, vmem_limit_bytes=66_000_000),
    )(old_section_of, new_section_of, old_order.T, new_order.T, freq, pieces, tokens)

    swapped = flag[0, 0] == 1
    joined = jnp.where(swapped, jnp.concatenate([kv[1], kv[0]], axis=-1),
                       jnp.concatenate([kv[0], kv[1]], axis=-1))
    return shards[None], joined[None]


def solution(mesh):
    in_specs = (P("section", None, "fsdp", None), P("section", "fsdp", None), P(), P(), P(), P())
    out_specs = (P("section", "fsdp", None), P("section", "fsdp", None))
    return jax.shard_map(
        per_device, mesh=mesh, in_specs=in_specs, out_specs=out_specs, check_vma=False
    )
```

```python
import math

import jax
import jax.numpy as jnp
from jax import lax
from jax.experimental import pallas as pl
from jax.experimental.pallas import tpu as pltpu
from jax.sharding import PartitionSpec as P

HEAD_DIM = 128
MESH = pl.DeviceIdType.MESH
NC = 8
NG = 4
TU = 8
SPLIT = 192


def body(oldsec, newsec, oldord, neword, freq, pieces, tokens, kv_out, shard_out,
         px, pc, og, cand, gb, wb, n2, sha, shb, xb, acc, ob, kvb, ct, st,
         pc_sem, rs, rr, zs, zr, xs, xr, ns, nr, shl, shs, shr,
         tl, tas, tar, ts, tr, tfs, tfr, osm, orm, kvs):
    rows = pieces.shape[1]
    cw = pieces.shape[2] // NC
    gw = pieces.shape[2] // NG
    per = NC // NG
    tok_rows, width = tokens.shape
    layers = oldsec.shape[0]
    s = lax.axis_index("section")
    m = lax.axis_index("fsdp")
    y = s // 2
    c = s % 2
    j = m // 16
    x = (m // 4) % 4
    z = m % 4
    h = z % 2
    zh = z // 2
    prob = (j + zh) % 2
    is_a = c == prob
    is_b = c != prob
    alone = jnp.logical_and(c == j, zh == 0)
    not_alone = jnp.logical_or(c != j, zh != 0)

    def dev(yy, cc, jj, xx, zz):
        return (2 * yy + cc, jj * 16 + xx * 4 + zz)

    core_dev = dev(y, 1 - c, j, x, z)
    cross_dev = [dev(1 - y, k, 1 - j, x, z) for k in range(2)]
    zf = (z + 2) % 4
    xp, xm, xf = (x + 1) % 4, (x + 3) % 4, (x + 2) % 4
    xp_dev, xm_dev = (dev(y, c, j, xx, z) for xx in (xp, xm))

    def remote(src, dst, send, recv, device):
        return pltpu.make_async_remote_copy(
            src_ref=src, dst_ref=dst, send_sem=send, recv_sem=recv,
            device_id=device, device_id_type=MESH)

    def arrived(dst, send, recv, device):
        remote(dst, dst, send, recv, device).wait_recv()

    def pc_copy(i, a):
        to = px.at[x, a] if i == 0 else pc.at[i, a]
        return pltpu.make_async_copy(pieces.at[a, :, pl.ds(i * cw, cw)], to, pc_sem.at[i, a])

    for i in range(NC):
        for a in range(2):
            pc_copy(i, a).start()

    def layer_of(section):
        found = jnp.int32(0)
        for l in range(layers):
            found = found + jnp.where(newsec[l] == section, l, 0)
        return found

    def entry(table, layer):
        found = jnp.int32(0)
        for l in range(layers):
            found = found + jnp.where(layer == l, table(l), 0)
        return found

    high = jnp.int32(0)
    for l in range(layers):
        high = jnp.where(oldsec[l] == s, l, high)
    row_high = entry(lambda l: newsec[l], high) // 2
    source = [entry(lambda l: oldsec[l], layer_of(2 * s + k)) for k in range(2)]
    gl = layer_of(2 * (2 * y + prob) + h)
    gl_crossed = jnp.where(entry(lambda l: oldsec[l], gl) // 2 == y, 0, 1)
    gl_old = entry(lambda l: oldord[0, l], gl)
    gl_new = entry(lambda l: neword[0, l], gl)
    gl_turn = (jnp.where(gl_old == gl_new, 0, 1) + gl_crossed + j + c) % 2
    is_key = gl_old == (c + gl_crossed) % 2
    ol = layer_of(2 * s + h)
    ol_crossed = jnp.where(entry(lambda l: oldsec[l], ol) // 2 == y, 0, 1)
    key_at = (entry(lambda l: oldord[0, l], ol) + ol_crossed) % 2

    barrier = pltpu.get_barrier_semaphore()
    partners = cross_dev + [xp_dev, xm_dev]
    for n in range(1, 16):
        partners.append(dev(y, (c + n) % 2, (j + n // 2) % 2, x, (z + n // 4) % 4))
    for device in partners:
        pl.semaphore_signal(barrier, inc=1, device_id=device, device_id_type=MESH)
    pl.semaphore_wait(barrier, len(partners))

    tok_step = width // (2 * TU)
    quarter = width // 4

    slots = [x, xm, xp, xf]

    def tok_cols(u, a):
        start = slots[u // 2] * quarter + (2 * a + u % 2) * tok_step
        return pl.ds(pl.multiple_of(start, tok_step), tok_step)

    def tok_send(v):
        u, a = v // 2, v % 2
        cols = tok_cols(u, a)
        parts = [(pl.ds(0, SPLIT), dev(y, a, 1 - j, x, z)),
                 (pl.ds(SPLIT, tok_rows - SPLIT), dev(y, a, j, x, zf))]
        return [remote(tokens.at[part, cols], xb.at[1, part, cols], ts.at[v, k], tr.at[u, k], device)
                for k, (part, device) in enumerate(parts)]

    def tok_here(u):
        cols = tok_cols(u, c)
        for k, part in enumerate((pl.ds(0, SPLIT), pl.ds(SPLIT, tok_rows - SPLIT))):
            arrived(xb.at[1, part, cols], tfs.at[u], tr.at[u, k], core_dev)

    def tok_pass(u):
        cols = tok_cols(u, c)
        return remote(xb.at[1, :, cols], xb.at[1, :, cols], tfs.at[u], tfr.at[u], core_dev)

    def tok_other(u):
        cols = tok_cols(u, 1 - c)
        return remote(xb.at[1, :, cols], xb.at[1, :, cols], tfs.at[u], tfr.at[u], core_dev)

    def tok_core(k):
        cols = pl.ds(k * quarter, quarter)
        return remote(tokens.at[:, cols], xb.at[0, :, cols], tas.at[k], tar.at[k], core_dev)

    tok_local = pltpu.make_async_copy(tokens, xb.at[0], tl.at[0])
    tok_next = [0]

    def send_tokens(count):
        take = range(tok_next[0], min(tok_next[0] + count, 2 * TU))
        tok_next[0] += len(take)

        @pl.when(is_b)
        def _():
            for v in take:
                for copy in tok_send(v):
                    copy.start()

    def relay_copies(e):
        return [remote(og.at[e, k], cand.at[e, s], rs.at[e, k],
                       rr.at[e, 0] if k == 0 else rr.at[e, 1 + c], device)
                for k, device in enumerate([core_dev] + cross_dev)]

    relay_rows = [2 * y + 1 - c, 2 * (1 - y), 2 * (1 - y) + 1]
    first_entries = [0] + [NC + k for k in range(3)]

    def relay(e, of):
        def tile(t, carry):
            part = pl.ds(pl.multiple_of(t * 128, 128), 128)
            low_rows, high_rows = of(0, part), of(1, part)
            for k in range(3):
                og[e, k, part, :] = jnp.where(row_high == relay_rows[k], high_rows, low_rows)
            cand[e, s, part, :] = jnp.where(row_high == s, high_rows, low_rows)
            return carry

        lax.fori_loop(0, rows // 128, tile, 0)
        for copy in relay_copies(e):
            copy.start()

    def relay_send(i):
        for a in range(2):
            pc_copy(i, a).wait()
        relay(i, lambda a, part: pc[i, a, part, :])

    def relay_first(b):
        relay(first_entries[b], lambda a, part: px[slots[b], a, part, :])

    def place(slot, zz):
        return pl.ds(pl.multiple_of((slots[slot] * 4 + zz) * rows, rows), rows)

    def spread(i, slot):
        copies = []
        for k in range(2):
            src = gb.at[slots[slot], k] if i == 0 else pc.at[i, k]
            target = 2 * ((c + j) % 2) + k
            for far in (1, 0):
                device = dev(y, j, (j + far) % 2, x, (target + 2 * far) % 4)
                copy = remote(src, wb.at[i, place(slot, z)], zs.at[i, slot, 2 * k + far],
                              zr.at[i, slot, z], device)
                here = jnp.logical_and(alone, h == k)
                copies.append((copy, None if far else jnp.logical_not(here)))
        return copies

    def spread_each(i, slot, act):
        for copy, needed in spread(i, slot):
            if needed is None:
                act(copy)
            else:
                @pl.when(needed)
                def _():
                    act(copy)

    def spread_start(i, slot):
        spread_each(i, slot, lambda copy: copy.start())

    def spread_arrived(i, slot):
        for n in range(1, 4):
            zz = (z + n) % 4
            arrived(wb.at[i, place(slot, zz)], zs.at[i, slot, 0], zr.at[i, slot, zz], core_dev)

        @pl.when(not_alone)
        def _():
            arrived(wb.at[i, place(slot, z)], zs.at[i, slot, 0], zr.at[i, slot, z], core_dev)

    def choose_from(e, i, slot, to):
        arrived(cand.at[e, 2 * y + 1 - c], rs.at[e, 0], rr.at[e, 0], core_dev)
        for k in range(2):
            arrived(cand.at[e, 2 * (1 - y) + k], rs.at[e, 1 + k], rr.at[e, 1 + k], cross_dev[k])

        def tile(t, carry):
            part = pl.ds(pl.multiple_of(t * 128, 128), 128)
            four = [cand[e, k, part, :] for k in range(4)]
            for k in range(2):
                want = source[k]
                to[k, part, :] = jnp.where(want < 2, jnp.where(want == 0, four[0], four[1]),
                                           jnp.where(want == 2, four[2], four[3]))
            return carry

        lax.fori_loop(0, rows // 128, tile, 0)
        spread_start(i, slot)

        @pl.when(alone)
        def _():
            def keep(t, carry):
                part = pl.ds(pl.multiple_of(t * 128, 128), 128)
                here = pl.ds(pl.multiple_of((slots[slot] * 4 + z) * rows + t * 128, 128), 128)
                wb[i, here, :] = to[h, part, :]
                return carry

            lax.fori_loop(0, rows // 128, keep, 0)

    def choose(i):
        choose_from(i, i, 0, pc.at[i])

    def choose_first(b):
        choose_from(first_entries[b], 0, b, gb.at[slots[b]])

    def first_own_copies():
        mine = px.at[x]
        return [remote(mine, mine, xs.at[0, 0], xr.at[0, 0], xp_dev),
                remote(mine, mine, xs.at[0, 1], xr.at[0, 1], xm_dev)]

    def first_pass_copies():
        left, right = px.at[xm, 0], px.at[xp, 1]
        return [remote(left, left, xs.at[0, 2], xr.at[0, 2], xp_dev),
                remote(right, right, xs.at[0, 3], xr.at[0, 3], xm_dev)]

    def first_own():
        for a in range(2):
            pc_copy(0, a).wait()
        for copy in first_own_copies():
            copy.start()

    def first_pass():
        arrived(px.at[xm], xs.at[0, 0], xr.at[0, 0], xp_dev)
        arrived(px.at[xp], xs.at[0, 1], xr.at[0, 1], xm_dev)
        for copy in first_pass_copies():
            copy.start()

    def first_far():
        arrived(px.at[xf, 0], xs.at[0, 2], xr.at[0, 2], xp_dev)
        arrived(px.at[xf, 1], xs.at[0, 3], xr.at[0, 3], xm_dev)

    def block(i, xx, first, count):
        return wb.at[i, pl.ds(pl.multiple_of(xx * 4 * rows + first, rows), count)]

    def own_copies(i):
        mine = block(i, x, 0, 4 * rows)
        return [remote(mine, mine, xs.at[i, 0], xr.at[i, 0], xp_dev),
                remote(mine, mine, xs.at[i, 1], xr.at[i, 1], xm_dev)]

    def pass_copies(i):
        left = block(i, xm, 0, 2 * rows)
        right = block(i, xp, 2 * rows, 2 * rows)
        return [remote(left, left, xs.at[i, 2], xr.at[i, 2], xp_dev),
                remote(right, right, xs.at[i, 3], xr.at[i, 3], xm_dev)]

    pair = pl.ds(pl.multiple_of((x * 4 + z // 2 * 2) * rows, rows), 2 * rows)

    def near_copy(i):
        return remote(wb.at[i, pair], n2.at[i], ns.at[i], nr.at[i], core_dev)

    def x_own(i):
        spread_arrived(i, 0)
        if i > 0:
            for copy in own_copies(i):
                copy.start()

        @pl.when(is_b)
        def _():
            near_copy(i).start()

    def x_pass(i):
        arrived(block(i, xm, 0, 4 * rows), xs.at[i, 0], xr.at[i, 0], xp_dev)
        first, second = pass_copies(i)
        first.start()
        arrived(block(i, xp, 0, 4 * rows), xs.at[i, 1], xr.at[i, 1], xm_dev)
        second.start()

    def far_arrived(i):
        if i == 0:
            for slot in (1, 2, 3):
                spread_arrived(i, slot)
            return
        arrived(block(i, xf, 0, 2 * rows), xs.at[i, 2], xr.at[i, 2], xp_dev)
        arrived(block(i, xf, 2 * rows, 2 * rows), xs.at[i, 3], xr.at[i, 3], xm_dev)

    def shard_local(i):
        return pltpu.make_async_copy(sha.at[i], shard_out.at[:, pl.ds(i * cw, cw)], shl.at[i])

    def shard_far(i):
        return remote(shb.at[i], shard_out.at[:, pl.ds(i * cw, cw)], shs.at[i], shr.at[i],
                      dev(y, c, 1 - j, x, z))

    def shard(i):
        @pl.when(is_a)
        def _():
            near_copy(i).wait_recv()

            def tile(t, carry):
                part = pl.ds(pl.multiple_of(t * 128, 128), 128)
                near = pl.ds(pl.multiple_of((x * 4 + z // 2 * 2) * rows + t * 128, 128), 128)
                mine = wb[i, near, :]
                other = n2[i, part, :]
                sha[i, part, :] = jnp.where(gl_turn == 0, mine, other)
                shb[i, part, :] = jnp.where(gl_turn == 0, other, mine)
                return carry

            lax.fori_loop(0, 2 * rows // 128, tile, 0)

    def shard_send(i):
        @pl.when(is_a)
        def _():
            shard_local(i).start()
            shard_far(i).start()

    def multiply(g, slots_now, xx, half):
        first = pl.multiple_of(xx * 4 * rows + half * 2 * rows, 2 * rows)
        ks = pl.ds(first, 2 * rows)
        weight = jnp.concatenate([wb[per * g + k, ks, :] for k in range(per)], axis=1)
        for slot in slots_now:
            acc[g, slot] += jnp.dot(xb[slot, :, ks], weight, preferred_element_type=jnp.float32)

    def clear(g):
        acc[g] = jnp.zeros(acc.shape[1:], acc.dtype)

    def near(g, slots_now, start, stop):
        def near_block(t, carry):
            b = t // 2
            multiply(g, slots_now, (x + 3 * b - b // 2 * 5) % 4, t % 2)
            return carry

        lax.fori_loop(2 * start, 2 * stop, near_block, 0)

    def far(g, slots_now):
        def far_block(t, carry):
            multiply(g, slots_now, xf, t)
            return carry

        lax.fori_loop(0, 2, far_block, 0)

    def finish(g, slot):
        def tile(t, carry):
            part = pl.ds(pl.multiple_of(t * 128, 128), 128)
            cosine = ct[slot, part, :]
            sine = st[slot, part, :]
            for head in range(gw // HEAD_DIM):
                cols = slice(head * HEAD_DIM, (head + 1) * HEAD_DIM)
                value = acc[g, slot, part, cols]
                turned = value * cosine + pltpu.roll(value, HEAD_DIM // 2, 1) * sine
                ob[g, slot, part, cols] = turned.astype(jnp.bfloat16)
            return carry

        lax.fori_loop(0, tok_rows // 128, tile, 0)

    def kv_part(g, q, part):
        return kvb.at[q, part, pl.ds(g * gw, gw)]

    all_rows = pl.ds(0, tok_rows)
    y_rows, z_rows = pl.ds(0, SPLIT), pl.ds(SPLIT, tok_rows - SPLIT)

    def out_near(g):
        return remote(ob.at[g, 0], kv_part(g, c, all_rows), osm.at[g, 0], orm.at[g, c], core_dev)

    def out_far(g):
        return [remote(ob.at[g, 1, y_rows], kv_part(g, c, y_rows), osm.at[g, 1], orm.at[g, c],
                       dev(y, prob, 1 - j, x, z)),
                remote(ob.at[g, 1, z_rows], kv_part(g, c, z_rows), osm.at[g, 2], orm.at[g, 2 + c],
                       dev(y, prob, j, x, zf))]

    def send_far(g):
        for copy in out_far(g):
            copy.start()

    def send_near(g):
        @pl.when(is_a)
        def _():
            def tile(t, carry):
                part = pl.ds(pl.multiple_of(t * 128, 128), 128)
                kvb[c, part, g * gw:(g + 1) * gw] = ob[g, 0, part, :]
                return carry

            lax.fori_loop(0, tok_rows // 128, tile, 0)

        @pl.when(is_b)
        def _():
            out_near(g).start()

    def stage(n):
        return cand.at[1 + n // 4, n % 4]

    def kv_copies(g):
        copies = []
        for n in range(2 * per):
            k, part = n // per, n % per
            cols = pl.ds(k * NG * gw + g * gw + part * cw, cw)
            copies.append(pltpu.make_async_copy(stage(2 * per * g + n), kv_out.at[:, cols],
                                                kvs.at[g, n]))
        return copies

    def collect(g):
        @pl.when(is_a)
        def _():
            arrived(kv_part(g, 1 - c, all_rows), osm.at[g, 0], orm.at[g, 1 - c], core_dev)

        @pl.when(is_b)
        def _():
            for q in range(2):
                arrived(kv_part(g, q, y_rows), osm.at[g, 0], orm.at[g, q], core_dev)
                arrived(kv_part(g, q, z_rows), osm.at[g, 0], orm.at[g, 2 + q], core_dev)

        def tile(t, carry):
            rows_now = pl.ds(pl.multiple_of(t * 128, 128), 128)
            for part in range(per):
                cols = slice(g * gw + part * cw, g * gw + (part + 1) * cw)
                first, second = kvb[0, rows_now, cols], kvb[1, rows_now, cols]
                stage(2 * per * g + part)[rows_now, :] = jnp.where(key_at == 0, first, second)
                stage(2 * per * g + per + part)[rows_now, :] = jnp.where(key_at == 0, second, first)
            return carry

        lax.fori_loop(0, tok_rows // 128, tile, 0)
        for copy in kv_copies(g):
            copy.start()

    def tables():
        first = m // 2 * tok_rows
        by_y = (m // 2 + 8) % 16 * tok_rows
        by_z = (m // 2 + 1 - 2 * zh) * tok_rows
        lane = lax.broadcasted_iota(jnp.int32, (64, HEAD_DIM), 1)
        row = lax.broadcasted_iota(jnp.int32, (64, HEAD_DIM), 0)

        def tile(t, carry):
            part = pl.ds(pl.multiple_of(t * 64, 64), 64)
            for slot in range(2):
                base = first if slot == 0 else jnp.where(t * 64 < SPLIT, by_y, by_z)
                position = (base + t * 64 + row).astype(jnp.float32)
                angle = position * freq[0:1, :]
                sine = jnp.sin(angle)
                sine = jnp.where(lane < HEAD_DIM // 2, -sine, sine)
                ct[slot, part, :] = jnp.where(is_key, jnp.cos(angle), 1.0)
                st[slot, part, :] = jnp.where(is_key, sine, 0.0)
            return carry

        lax.fori_loop(0, tok_rows // 64, tile, 0)

    def token_pass(u):
        tok_here(u)
        tok_pass(u).start()

    def token_other(b):
        for u in (2 * b, 2 * b + 1):
            tok_other(u).wait_recv()

    first_own()
    for i in range(1, NC):
        relay_send(i)
    send_tokens(1)
    choose(1)
    first_pass()
    choose(2)
    x_own(1)
    first_far()
    for b in range(4):
        relay_first(b)
    choose(3)
    x_own(2)

    @pl.when(is_a)
    def _():
        tok_local.start()
        for k in range(4):
            tok_core(k).start()

    choose(4)
    x_own(3)
    x_pass(1)
    choose(5)
    x_own(4)
    choose(6)
    x_own(5)
    choose(7)
    send_tokens(2 * TU)
    x_own(6)
    x_pass(2)
    x_own(7)
    tables()

    @pl.when(is_a)
    def _():
        tok_local.wait()

    @pl.when(is_b)
    def _():
        for k in range(4):
            tok_core(k).wait_recv()

    for g in range(NG):
        clear(g)
    x_pass(3)
    for b in range(4):
        choose_first(b)
    near(1, (0,), 0, 3)
    token_pass(0)
    x_pass(4)
    token_pass(1)
    token_pass(2)
    token_other(0)
    near(1, (1,), 0, 1)
    x_pass(5)
    token_pass(3)
    near(2, (0,), 0, 3)
    token_pass(4)
    x_pass(6)
    token_other(1)
    near(1, (1,), 1, 2)
    near(2, (1,), 0, 2)
    token_pass(5)
    x_pass(7)
    for i in range(1, 5):
        shard(i)
        shard_send(i)
    for i in range(5, 8):
        shard(i)
        shard_send(i)
    near(3, (0,), 0, 3)
    token_pass(6)
    token_other(2)
    for g in (1, 2):
        near(g, (1,), 2, 3)
    near(3, (1,), 0, 3)
    token_pass(7)
    token_other(3)
    x_own(0)
    for g in (1, 2, 0, 3):
        for k in range(per):
            far_arrived(per * g + k)
        if g == 0:
            shard(0)
            shard_send(0)
            near(g, (0, 1), 0, 3)
        if g == 3:
            far(g, (1,))
            finish(g, 1)
            send_far(g)
            far(g, (0,))
            finish(g, 0)
            send_near(g)
        else:
            far(g, (0, 1))
            finish(g, 1)
            send_far(g)
            finish(g, 0)
            send_near(g)
        if g == 0:
            collect(1)
    for g in (2, 0, 3):
        collect(g)

    for e in list(range(NC)) + first_entries[1:]:
        for copy in relay_copies(e):
            copy.wait_send()
    for i in range(NC):
        for copy in first_own_copies() + first_pass_copies() if i == 0 else own_copies(i) + pass_copies(i):
            copy.wait_send()
        for slot in range(4 if i == 0 else 1):
            spread_each(i, slot, lambda copy: copy.wait_send())

    @pl.when(is_a)
    def _():
        for k in range(4):
            tok_core(k).wait_send()
        for i in range(NC):
            shard_local(i).wait()
            shard_far(i).wait_send()

    @pl.when(is_b)
    def _():
        for v in range(2 * TU):
            for copy in tok_send(v):
                copy.wait_send()
        for i in range(NC):
            near_copy(i).wait_send()
            shard_far(i).wait_recv()
        for g in range(NG):
            out_near(g).wait_send()

    for u in range(TU):
        tok_pass(u).wait_send()
    for g in range(NG):
        for copy in out_far(g):
            copy.wait_send()
        for copy in kv_copies(g):
            copy.wait()


def per_device(old_pieces, section_inputs, old_section_of, new_section_of, old_order, new_order):
    pieces = old_pieces[0]
    tokens = section_inputs[0]
    _, rows, kv_width = pieces.shape
    tok_rows, width = tokens.shape
    cw, gw = kv_width // NC, kv_width // NG

    half_dim = HEAD_DIM // 2
    freq_index = (jnp.arange(HEAD_DIM, dtype=jnp.int32) % half_dim).astype(jnp.float32)
    inverse_freq = jnp.exp(freq_index * (-2.0 * math.log(500000.0) / HEAD_DIM))
    freq = jnp.broadcast_to(inverse_freq[None, :], (8, HEAD_DIM))

    dma = pltpu.SemaphoreType.DMA
    bf, fl = jnp.bfloat16, jnp.float32
    hbm = pl.BlockSpec(memory_space=pltpu.HBM)
    vmem = pl.BlockSpec(memory_space=pltpu.VMEM)
    smem = pl.BlockSpec(memory_space=pltpu.SMEM)
    kv, shards = pl.pallas_call(
        body,
        out_shape=(jax.ShapeDtypeStruct((tok_rows, 2 * kv_width), bf),
                   jax.ShapeDtypeStruct((2 * rows, kv_width), bf)),
        in_specs=[smem] * 4 + [vmem] + [hbm] * 2,
        out_specs=(hbm, hbm),
        scratch_shapes=[
            pltpu.VMEM((4, 2, rows, cw), bf),
            pltpu.VMEM((NC, 2, rows, cw), bf),
            pltpu.VMEM((NC + 3, 3, rows, cw), bf),
            pltpu.VMEM((NC + 3, 4, rows, cw), bf),
            pltpu.VMEM((4, 2, rows, cw), bf),
            pltpu.VMEM((NC, width, cw), bf),
            pltpu.VMEM((NC, 2 * rows, cw), bf),
            pltpu.VMEM((NC, 2 * rows, cw), bf),
            pltpu.VMEM((NC, 2 * rows, cw), bf),
            pltpu.VMEM((2, tok_rows, width), bf),
            pltpu.VMEM((NG, 2, tok_rows, gw), fl),
            pltpu.VMEM((NG, 2, tok_rows, gw), bf),
            pltpu.VMEM((2, tok_rows, kv_width), bf),
            pltpu.VMEM((2, tok_rows, HEAD_DIM), fl),
            pltpu.VMEM((2, tok_rows, HEAD_DIM), fl),
            dma((NC, 2)), dma((NC + 3, 3)), dma((NC + 3, 3)),
            dma((NC, 4, 4)), dma((NC, 4, 4)), dma((NC, 4)), dma((NC, 4)),
            dma((NC,)), dma((NC,)), dma((NC,)), dma((NC,)), dma((NC,)),
            dma((1,)), dma((4,)), dma((4,)), dma((2 * TU, 2)), dma((TU, 2)), dma((TU,)), dma((TU,)),
            dma((NG, 3)), dma((NG, 4)), dma((NG, 2 * NC // NG)),
        ],
        compiler_params=pltpu.CompilerParams(
            collective_id=0, has_side_effects=True, vmem_limit_bytes=66_000_000),
    )(old_section_of, new_section_of, old_order.T, new_order.T, freq, pieces, tokens)

    return shards[None], kv[None]


def solution(mesh):
    in_specs = (P("section", None, "fsdp", None), P("section", "fsdp", None), P(), P(), P(), P())
    out_specs = (P("section", "fsdp", None), P("section", "fsdp", None))
    return jax.shard_map(
        per_device, mesh=mesh, in_specs=in_specs, out_specs=out_specs, check_vma=False
    )
```

```python
import math

import jax
import jax.numpy as jnp
from jax import lax
from jax.experimental import pallas as pl
from jax.experimental.pallas import tpu as pltpu
from jax.sharding import PartitionSpec as P

HEAD_DIM = 128
MESH = pl.DeviceIdType.MESH
NC = 8
NG = 4
TU = 8
SPLIT = 224


def body(oldsec, newsec, oldord, neword, freq, pieces, tokens, kv_out, shard_out,
         px, pc, og, cand, gb, wb, n2, sha, shb, xb, acc, ob, kvb, ct, st,
         pc_sem, rs, rr, zs, zr, xs, xr, ns, nr, shl, shs, shr,
         tl, tas, tar, ts, tr, tfs, tfr, osm, orm, kvs, xs1, xr1):
    rows = pieces.shape[1]
    cw = pieces.shape[2] // NC
    gw = pieces.shape[2] // NG
    per = NC // NG
    tok_rows, width = tokens.shape
    layers = oldsec.shape[0]
    s = lax.axis_index("section")
    m = lax.axis_index("fsdp")
    y = s // 2
    c = s % 2
    j = m // 16
    x = (m // 4) % 4
    z = m % 4
    h = z % 2
    zh = z // 2
    prob = (j + zh) % 2
    is_a = c == prob
    is_b = c != prob
    alone = jnp.logical_and(c == j, zh == 0)
    not_alone = jnp.logical_or(c != j, zh != 0)

    def dev(yy, cc, jj, xx, zz):
        return (2 * yy + cc, jj * 16 + xx * 4 + zz)

    core_dev = dev(y, 1 - c, j, x, z)
    cross_dev = [dev(1 - y, k, 1 - j, x, z) for k in range(2)]
    zf = (z + 2) % 4
    xp, xm, xf = (x + 1) % 4, (x + 3) % 4, (x + 2) % 4
    xp_dev, xm_dev = (dev(y, c, j, xx, z) for xx in (xp, xm))

    def remote(src, dst, send, recv, device):
        return pltpu.make_async_remote_copy(
            src_ref=src, dst_ref=dst, send_sem=send, recv_sem=recv,
            device_id=device, device_id_type=MESH)

    def arrived(dst, send, recv, device):
        remote(dst, dst, send, recv, device).wait_recv()

    def pc_copy(i, a):
        to = px.at[x, a] if i == 0 else pc.at[i, a]
        return pltpu.make_async_copy(pieces.at[a, :, pl.ds(i * cw, cw)], to, pc_sem.at[i, a])

    for i in range(NC):
        for a in range(2):
            pc_copy(i, a).start()

    def layer_of(section):
        found = jnp.int32(0)
        for l in range(layers):
            found = found + jnp.where(newsec[l] == section, l, 0)
        return found

    def entry(table, layer):
        found = jnp.int32(0)
        for l in range(layers):
            found = found + jnp.where(layer == l, table(l), 0)
        return found

    high = jnp.int32(0)
    for l in range(layers):
        high = jnp.where(oldsec[l] == s, l, high)
    row_high = entry(lambda l: newsec[l], high) // 2
    source = [entry(lambda l: oldsec[l], layer_of(2 * s + k)) for k in range(2)]
    gl = layer_of(2 * (2 * y + prob) + h)
    gl_crossed = jnp.where(entry(lambda l: oldsec[l], gl) // 2 == y, 0, 1)
    gl_old = entry(lambda l: oldord[0, l], gl)
    gl_new = entry(lambda l: neword[0, l], gl)
    gl_turn = (jnp.where(gl_old == gl_new, 0, 1) + gl_crossed + j + c) % 2
    is_key = gl_old == (c + gl_crossed) % 2
    ol = layer_of(2 * s + h)
    ol_crossed = jnp.where(entry(lambda l: oldsec[l], ol) // 2 == y, 0, 1)
    key_at = (entry(lambda l: oldord[0, l], ol) + ol_crossed) % 2

    barrier = pltpu.get_barrier_semaphore()
    partners = cross_dev + [xp_dev, xm_dev]
    for n in range(1, 16):
        partners.append(dev(y, (c + n) % 2, (j + n // 2) % 2, x, (z + n // 4) % 4))
    for device in partners:
        pl.semaphore_signal(barrier, inc=1, device_id=device, device_id_type=MESH)
    pl.semaphore_wait(barrier, len(partners))

    tok_step = width // (2 * TU)
    quarter = width // 4

    slots = [x, xm, xp, xf]

    def tok_cols(u, a):
        start = slots[u // 2] * quarter + (2 * a + u % 2) * tok_step
        return pl.ds(pl.multiple_of(start, tok_step), tok_step)

    def tok_send(v):
        u, a = v // 2, v % 2
        cols = tok_cols(u, a)
        parts = [(pl.ds(0, SPLIT), dev(y, a, 1 - j, x, z)),
                 (pl.ds(SPLIT, tok_rows - SPLIT), dev(y, a, j, x, zf))]
        return [remote(tokens.at[part, cols], xb.at[1, part, cols], ts.at[v, k], tr.at[u, k], device)
                for k, (part, device) in enumerate(parts)]

    def tok_here(u):
        cols = tok_cols(u, c)
        for k, part in enumerate((pl.ds(0, SPLIT), pl.ds(SPLIT, tok_rows - SPLIT))):
            arrived(xb.at[1, part, cols], tfs.at[u], tr.at[u, k], core_dev)

    def tok_pass(u):
        cols = tok_cols(u, c)
        return remote(xb.at[1, :, cols], xb.at[1, :, cols], tfs.at[u], tfr.at[u], core_dev)

    def tok_other(u):
        cols = tok_cols(u, 1 - c)
        return remote(xb.at[1, :, cols], xb.at[1, :, cols], tfs.at[u], tfr.at[u], core_dev)

    def tok_core(k):
        cols = pl.ds(k * quarter, quarter)
        return remote(tokens.at[:, cols], xb.at[0, :, cols], tas.at[k], tar.at[k], core_dev)

    tok_local = pltpu.make_async_copy(tokens, xb.at[0], tl.at[0])
    tok_next = [0]

    def send_tokens(count):
        take = range(tok_next[0], min(tok_next[0] + count, 2 * TU))
        tok_next[0] += len(take)

        @pl.when(is_b)
        def _():
            for v in take:
                for copy in tok_send(v):
                    copy.start()

    def relay_copies(e):
        return [remote(og.at[e, k], cand.at[e, s], rs.at[e, k],
                       rr.at[e, 0] if k == 0 else rr.at[e, 1 + c], device)
                for k, device in enumerate([core_dev] + cross_dev)]

    relay_rows = [2 * y + 1 - c, 2 * (1 - y), 2 * (1 - y) + 1]
    first_entries = [0] + [NC + k for k in range(3)]

    def relay(e, of):
        def tile(t, carry):
            part = pl.ds(pl.multiple_of(t * 128, 128), 128)
            low_rows, high_rows = of(0, part), of(1, part)
            for k in range(3):
                og[e, k, part, :] = jnp.where(row_high == relay_rows[k], high_rows, low_rows)
            cand[e, s, part, :] = jnp.where(row_high == s, high_rows, low_rows)
            return carry

        lax.fori_loop(0, rows // 128, tile, 0)
        for copy in relay_copies(e):
            copy.start()

    def relay_send(i):
        for a in range(2):
            pc_copy(i, a).wait()
        relay(i, lambda a, part: pc[i, a, part, :])

    def relay_first(b):
        relay(first_entries[b], lambda a, part: px[slots[b], a, part, :])

    def place(slot, zz):
        return pl.ds(pl.multiple_of((slots[slot] * 4 + zz) * rows, rows), rows)

    def spread(i, slot):
        copies = []
        for k in range(2):
            src = gb.at[slots[slot], k] if i == 0 else pc.at[i, k]
            target = 2 * ((c + j) % 2) + k
            for far in (1, 0):
                device = dev(y, j, (j + far) % 2, x, (target + 2 * far) % 4)
                copy = remote(src, wb.at[i, place(slot, z)], zs.at[i, slot, 2 * k + far],
                              zr.at[i, slot, z], device)
                here = jnp.logical_and(alone, h == k)
                copies.append((copy, None if far else jnp.logical_not(here)))
        return copies

    def spread_each(i, slot, act):
        for copy, needed in spread(i, slot):
            if needed is None:
                act(copy)
            else:
                @pl.when(needed)
                def _():
                    act(copy)

    def spread_start(i, slot):
        spread_each(i, slot, lambda copy: copy.start())

    def spread_arrived(i, slot):
        for n in range(1, 4):
            zz = (z + n) % 4
            arrived(wb.at[i, place(slot, zz)], zs.at[i, slot, 0], zr.at[i, slot, zz], core_dev)

        @pl.when(not_alone)
        def _():
            arrived(wb.at[i, place(slot, z)], zs.at[i, slot, 0], zr.at[i, slot, z], core_dev)

    def choose_from(e, i, slot, to):
        arrived(cand.at[e, 2 * y + 1 - c], rs.at[e, 0], rr.at[e, 0], core_dev)
        for k in range(2):
            arrived(cand.at[e, 2 * (1 - y) + k], rs.at[e, 1 + k], rr.at[e, 1 + k], cross_dev[k])

        def tile(t, carry):
            part = pl.ds(pl.multiple_of(t * 128, 128), 128)
            four = [cand[e, k, part, :] for k in range(4)]
            for k in range(2):
                want = source[k]
                to[k, part, :] = jnp.where(want < 2, jnp.where(want == 0, four[0], four[1]),
                                           jnp.where(want == 2, four[2], four[3]))
            return carry

        lax.fori_loop(0, rows // 128, tile, 0)
        spread_start(i, slot)

        @pl.when(alone)
        def _():
            def keep(t, carry):
                part = pl.ds(pl.multiple_of(t * 128, 128), 128)
                here = pl.ds(pl.multiple_of((slots[slot] * 4 + z) * rows + t * 128, 128), 128)
                wb[i, here, :] = to[h, part, :]
                return carry

            lax.fori_loop(0, rows // 128, keep, 0)

    def choose(i):
        choose_from(i, i, 0, pc.at[i])

    def choose_first(b):
        choose_from(first_entries[b], 0, b, gb.at[slots[b]])

    def first_own_copies():
        mine = px.at[x]
        return [remote(mine, mine, xs.at[0, 0], xr.at[0, 0], xp_dev),
                remote(mine, mine, xs.at[0, 1], xr.at[0, 1], xm_dev)]

    def first_pass_copies():
        left, right = px.at[xm, 0], px.at[xp, 1]
        return [remote(left, left, xs.at[0, 2], xr.at[0, 2], xp_dev),
                remote(right, right, xs.at[0, 3], xr.at[0, 3], xm_dev)]

    def first_own():
        for a in range(2):
            pc_copy(0, a).wait()
        for copy in first_own_copies():
            copy.start()

    def first_pass():
        arrived(px.at[xm], xs.at[0, 0], xr.at[0, 0], xp_dev)
        arrived(px.at[xp], xs.at[0, 1], xr.at[0, 1], xm_dev)
        for copy in first_pass_copies():
            copy.start()

    def first_far():
        arrived(px.at[xf, 0], xs.at[0, 2], xr.at[0, 2], xp_dev)
        arrived(px.at[xf, 1], xs.at[0, 3], xr.at[0, 3], xm_dev)

    def block(i, xx, first, count):
        return wb.at[i, pl.ds(pl.multiple_of(xx * 4 * rows + first, rows), count)]

    def own_copies(i):
        mine = block(i, x, 0, 4 * rows)
        return [remote(mine, mine, xs.at[i, 0], xr.at[i, 0], xp_dev),
                remote(mine, mine, xs.at[i, 1], xr.at[i, 1], xm_dev)]

    def pass_copies(i):
        left = block(i, xm, 0, 2 * rows)
        right = block(i, xp, 2 * rows, 2 * rows)
        return [remote(left, left, xs.at[i, 2], xr.at[i, 2], xp_dev),
                remote(right, right, xs.at[i, 3], xr.at[i, 3], xm_dev)]

    pair = pl.ds(pl.multiple_of((x * 4 + z // 2 * 2) * rows, rows), 2 * rows)

    def near_copy(i):
        return remote(wb.at[i, pair], n2.at[i], ns.at[i], nr.at[i], core_dev)

    def x_own(i):
        spread_arrived(i, 0)
        if i > 0:
            for copy in own_copies(i):
                copy.start()

        @pl.when(is_b)
        def _():
            near_copy(i).start()

    def own_pieces(zz):
        mine = wb.at[1, place(0, zz)]
        return [remote(mine, mine, xs1.at[0, zz], xr1.at[0, zz], xp_dev),
                remote(mine, mine, xs1.at[1, zz], xr1.at[1, zz], xm_dev)]

    def x_arrived(i, side, slot, device):
        if i == 1:
            for zz in range(4):
                arrived(wb.at[1, place(slot, zz)], xs1.at[side, zz], xr1.at[side, zz], device)
        else:
            arrived(block(i, slots[slot], 0, 4 * rows), xs.at[i, side], xr.at[i, side], device)

    def x_own_first():
        for n in (0, 1, 3, 2):
            zz = (z + n) % 4
            if n == 0:
                @pl.when(not_alone)
                def _():
                    arrived(wb.at[1, place(0, z)], zs.at[1, 0, 0], zr.at[1, 0, z], core_dev)
            else:
                arrived(wb.at[1, place(0, zz)], zs.at[1, 0, 0], zr.at[1, 0, zz], core_dev)
            for copy in own_pieces(zz):
                copy.start()

        @pl.when(is_b)
        def _():
            near_copy(1).start()

    def x_pass(i):
        x_arrived(i, 0, 1, xp_dev)
        first, second = pass_copies(i)
        first.start()
        x_arrived(i, 1, 2, xm_dev)
        second.start()

    def far_arrived(i):
        if i == 0:
            for slot in (1, 2, 3):
                spread_arrived(i, slot)
            return
        arrived(block(i, xf, 0, 2 * rows), xs.at[i, 2], xr.at[i, 2], xp_dev)
        arrived(block(i, xf, 2 * rows, 2 * rows), xs.at[i, 3], xr.at[i, 3], xm_dev)

    def shard_local(i):
        return pltpu.make_async_copy(sha.at[i], shard_out.at[:, pl.ds(i * cw, cw)], shl.at[i])

    def shard_far(i):
        return remote(shb.at[i], shard_out.at[:, pl.ds(i * cw, cw)], shs.at[i], shr.at[i],
                      dev(y, c, 1 - j, x, z))

    def shard(i):
        @pl.when(is_a)
        def _():
            near_copy(i).wait_recv()

            def tile(t, carry):
                part = pl.ds(pl.multiple_of(t * 128, 128), 128)
                near = pl.ds(pl.multiple_of((x * 4 + z // 2 * 2) * rows + t * 128, 128), 128)
                mine = wb[i, near, :]
                other = n2[i, part, :]
                sha[i, part, :] = jnp.where(gl_turn == 0, mine, other)
                shb[i, part, :] = jnp.where(gl_turn == 0, other, mine)
                return carry

            lax.fori_loop(0, 2 * rows // 128, tile, 0)

    def shard_send(i):
        @pl.when(is_a)
        def _():
            shard_local(i).start()
            shard_far(i).start()

    def multiply(g, slots_now, xx, half):
        first = pl.multiple_of(xx * 4 * rows + half * 2 * rows, 2 * rows)
        ks = pl.ds(first, 2 * rows)
        weight = jnp.concatenate([wb[per * g + k, ks, :] for k in range(per)], axis=1)
        for slot in slots_now:
            acc[g, slot] += jnp.dot(xb[slot, :, ks], weight, preferred_element_type=jnp.float32)

    def clear(g):
        acc[g] = jnp.zeros(acc.shape[1:], acc.dtype)

    def near(g, slots_now, start, stop):
        def near_block(t, carry):
            b = t // 2
            multiply(g, slots_now, (x + 3 * b - b // 2 * 5) % 4, t % 2)
            return carry

        lax.fori_loop(2 * start, 2 * stop, near_block, 0)

    def far(g, slots_now):
        def far_block(t, carry):
            multiply(g, slots_now, xf, t)
            return carry

        lax.fori_loop(0, 2, far_block, 0)

    def finish(g, slot):
        def tile(t, carry):
            part = pl.ds(pl.multiple_of(t * 128, 128), 128)
            cosine = ct[slot, part, :]
            sine = st[slot, part, :]
            for head in range(gw // HEAD_DIM):
                cols = slice(head * HEAD_DIM, (head + 1) * HEAD_DIM)
                value = acc[g, slot, part, cols]
                turned = value * cosine + pltpu.roll(value, HEAD_DIM // 2, 1) * sine
                ob[g, slot, part, cols] = turned.astype(jnp.bfloat16)
            return carry

        lax.fori_loop(0, tok_rows // 128, tile, 0)

    def kv_part(g, q, part):
        return kvb.at[q, part, pl.ds(g * gw, gw)]

    all_rows = pl.ds(0, tok_rows)
    y_rows, z_rows = pl.ds(0, SPLIT), pl.ds(SPLIT, tok_rows - SPLIT)

    def out_near(g):
        return remote(ob.at[g, 0], kv_part(g, c, all_rows), osm.at[g, 0], orm.at[g, c], core_dev)

    def out_far(g):
        return [remote(ob.at[g, 1, y_rows], kv_part(g, c, y_rows), osm.at[g, 1], orm.at[g, c],
                       dev(y, prob, 1 - j, x, z)),
                remote(ob.at[g, 1, z_rows], kv_part(g, c, z_rows), osm.at[g, 2], orm.at[g, 2 + c],
                       dev(y, prob, j, x, zf))]

    def send_far(g):
        for copy in out_far(g):
            copy.start()

    def send_near(g):
        @pl.when(is_a)
        def _():
            def tile(t, carry):
                part = pl.ds(pl.multiple_of(t * 128, 128), 128)
                kvb[c, part, g * gw:(g + 1) * gw] = ob[g, 0, part, :]
                return carry

            lax.fori_loop(0, tok_rows // 128, tile, 0)

        @pl.when(is_b)
        def _():
            out_near(g).start()

    def stage(n):
        return cand.at[1 + n // 4, n % 4]

    def kv_copies(g):
        copies = []
        for n in range(2 * per):
            k, part = n // per, n % per
            cols = pl.ds(k * NG * gw + g * gw + part * cw, cw)
            copies.append(pltpu.make_async_copy(stage(2 * per * g + n), kv_out.at[:, cols],
                                                kvs.at[g, n]))
        return copies

    def collect(g):
        @pl.when(is_a)
        def _():
            arrived(kv_part(g, 1 - c, all_rows), osm.at[g, 0], orm.at[g, 1 - c], core_dev)

        @pl.when(is_b)
        def _():
            for q in range(2):
                arrived(kv_part(g, q, y_rows), osm.at[g, 0], orm.at[g, q], core_dev)
                arrived(kv_part(g, q, z_rows), osm.at[g, 0], orm.at[g, 2 + q], core_dev)

        def tile(t, carry):
            rows_now = pl.ds(pl.multiple_of(t * 128, 128), 128)
            for part in range(per):
                cols = slice(g * gw + part * cw, g * gw + (part + 1) * cw)
                first, second = kvb[0, rows_now, cols], kvb[1, rows_now, cols]
                stage(2 * per * g + part)[rows_now, :] = jnp.where(key_at == 0, first, second)
                stage(2 * per * g + per + part)[rows_now, :] = jnp.where(key_at == 0, second, first)
            return carry

        lax.fori_loop(0, tok_rows // 128, tile, 0)
        for copy in kv_copies(g):
            copy.start()

    def tables():
        first = m // 2 * tok_rows
        by_y = (m // 2 + 8) % 16 * tok_rows
        by_z = (m // 2 + 1 - 2 * zh) * tok_rows
        lane = lax.broadcasted_iota(jnp.int32, (64, HEAD_DIM), 1)
        row = lax.broadcasted_iota(jnp.int32, (64, HEAD_DIM), 0)

        def tile(t, carry):
            part = pl.ds(pl.multiple_of(t * 64, 64), 64)
            for slot in range(2):
                base = first if slot == 0 else jnp.where(t * 64 + row < SPLIT, by_y, by_z)
                position = (base + t * 64 + row).astype(jnp.float32)
                angle = position * freq[0:1, :]
                sine = jnp.sin(angle)
                sine = jnp.where(lane < HEAD_DIM // 2, -sine, sine)
                ct[slot, part, :] = jnp.where(is_key, jnp.cos(angle), 1.0)
                st[slot, part, :] = jnp.where(is_key, sine, 0.0)
            return carry

        lax.fori_loop(0, tok_rows // 64, tile, 0)

    def token_pass(u):
        tok_here(u)
        tok_pass(u).start()

    def token_other(b):
        for u in (2 * b, 2 * b + 1):
            tok_other(u).wait_recv()

    def sent_copies(i):
        if i == 0:
            return first_own_copies() + first_pass_copies()
        if i == 1:
            return sum([own_pieces(zz) for zz in range(4)], pass_copies(1))
        return own_copies(i) + pass_copies(i)

    first_own()
    for i in range(1, NC):
        relay_send(i)
    send_tokens(1)
    choose(1)
    first_pass()
    choose(2)
    x_own_first()
    first_far()
    for b in range(4):
        relay_first(b)
    choose(3)
    x_own(2)

    @pl.when(is_a)
    def _():
        tok_local.start()
        for k in range(4):
            tok_core(k).start()

    choose(4)
    x_own(3)
    x_pass(1)
    choose(5)
    x_own(4)
    choose(6)
    x_own(5)
    choose(7)
    send_tokens(TU)
    x_own(6)
    x_pass(2)
    x_own(7)
    tables()

    @pl.when(is_a)
    def _():
        tok_local.wait()

    @pl.when(is_b)
    def _():
        for k in range(4):
            tok_core(k).wait_recv()

    for g in range(NG):
        clear(g)
    x_pass(3)
    for b in range(4):
        choose_first(b)
    send_tokens(2 * TU)
    near(1, (0,), 0, 3)
    token_pass(0)
    x_pass(4)
    token_pass(1)
    token_other(0)
    near(1, (1,), 0, 1)
    token_pass(2)
    token_pass(3)
    x_pass(5)
    token_other(1)
    near(1, (1,), 1, 2)
    near(2, (0,), 0, 3)
    near(2, (1,), 0, 2)
    x_pass(6)
    for i in range(1, 8):
        shard(i)
        shard_send(i)
    x_own(0)
    far_arrived(0)
    near(0, (0,), 0, 3)
    near(0, (1,), 0, 2)
    x_pass(7)
    near(3, (0,), 0, 3)
    shard(0)
    shard_send(0)
    token_pass(4)
    token_pass(5)
    token_other(2)
    near(0, (1,), 2, 3)
    near(1, (1,), 2, 3)
    near(2, (1,), 2, 3)
    near(3, (1,), 0, 3)
    far_arrived(1)
    far(0, (0,))
    far_arrived(2)
    far_arrived(3)
    far(1, (0,))
    token_pass(6)
    token_pass(7)
    token_other(3)
    for g in range(NG):
        if g >= 2:
            for k in range(per):
                far_arrived(per * g + k)
        far(g, (1,))
        finish(g, 1)
        send_far(g)
        if g >= 2:
            far(g, (0,))
        finish(g, 0)
        send_near(g)
    for g in range(NG):
        collect(g)

    for e in list(range(NC)) + first_entries[1:]:
        for copy in relay_copies(e):
            copy.wait_send()
    for i in range(NC):
        for copy in sent_copies(i):
            copy.wait_send()
        for slot in range(4 if i == 0 else 1):
            spread_each(i, slot, lambda copy: copy.wait_send())

    @pl.when(is_a)
    def _():
        for k in range(4):
            tok_core(k).wait_send()
        for i in range(NC):
            shard_local(i).wait()
            shard_far(i).wait_send()

    @pl.when(is_b)
    def _():
        for v in range(2 * TU):
            for copy in tok_send(v):
                copy.wait_send()
        for i in range(NC):
            near_copy(i).wait_send()
            shard_far(i).wait_recv()
        for g in range(NG):
            out_near(g).wait_send()

    for u in range(TU):
        tok_pass(u).wait_send()
    for g in range(NG):
        for copy in out_far(g):
            copy.wait_send()
        for copy in kv_copies(g):
            copy.wait()


def per_device(old_pieces, section_inputs, old_section_of, new_section_of, old_order, new_order):
    pieces = old_pieces[0]
    tokens = section_inputs[0]
    _, rows, kv_width = pieces.shape
    tok_rows, width = tokens.shape
    cw, gw = kv_width // NC, kv_width // NG

    half_dim = HEAD_DIM // 2
    freq_index = (jnp.arange(HEAD_DIM, dtype=jnp.int32) % half_dim).astype(jnp.float32)
    inverse_freq = jnp.exp(freq_index * (-2.0 * math.log(500000.0) / HEAD_DIM))
    freq = jnp.broadcast_to(inverse_freq[None, :], (8, HEAD_DIM))

    dma = pltpu.SemaphoreType.DMA
    bf, fl = jnp.bfloat16, jnp.float32
    hbm = pl.BlockSpec(memory_space=pltpu.HBM)
    vmem = pl.BlockSpec(memory_space=pltpu.VMEM)
    smem = pl.BlockSpec(memory_space=pltpu.SMEM)
    kv, shards = pl.pallas_call(
        body,
        out_shape=(jax.ShapeDtypeStruct((tok_rows, 2 * kv_width), bf),
                   jax.ShapeDtypeStruct((2 * rows, kv_width), bf)),
        in_specs=[smem] * 4 + [vmem] + [hbm] * 2,
        out_specs=(hbm, hbm),
        scratch_shapes=[
            pltpu.VMEM((4, 2, rows, cw), bf),
            pltpu.VMEM((NC, 2, rows, cw), bf),
            pltpu.VMEM((NC + 3, 3, rows, cw), bf),
            pltpu.VMEM((NC + 3, 4, rows, cw), bf),
            pltpu.VMEM((4, 2, rows, cw), bf),
            pltpu.VMEM((NC, width, cw), bf),
            pltpu.VMEM((NC, 2 * rows, cw), bf),
            pltpu.VMEM((NC, 2 * rows, cw), bf),
            pltpu.VMEM((NC, 2 * rows, cw), bf),
            pltpu.VMEM((2, tok_rows, width), bf),
            pltpu.VMEM((NG, 2, tok_rows, gw), fl),
            pltpu.VMEM((NG, 2, tok_rows, gw), bf),
            pltpu.VMEM((2, tok_rows, kv_width), bf),
            pltpu.VMEM((2, tok_rows, HEAD_DIM), fl),
            pltpu.VMEM((2, tok_rows, HEAD_DIM), fl),
            dma((NC, 2)), dma((NC + 3, 3)), dma((NC + 3, 3)),
            dma((NC, 4, 4)), dma((NC, 4, 4)), dma((NC, 4)), dma((NC, 4)),
            dma((NC,)), dma((NC,)), dma((NC,)), dma((NC,)), dma((NC,)),
            dma((1,)), dma((4,)), dma((4,)), dma((2 * TU, 2)), dma((TU, 2)), dma((TU,)), dma((TU,)),
            dma((NG, 3)), dma((NG, 4)), dma((NG, 2 * NC // NG)),
            dma((2, 4)), dma((2, 4)),
        ],
        compiler_params=pltpu.CompilerParams(
            collective_id=0, has_side_effects=True, vmem_limit_bytes=66_000_000),
    )(old_section_of, new_section_of, old_order.T, new_order.T, freq, pieces, tokens)

    return shards[None], kv[None]


def solution(mesh):
    in_specs = (P("section", None, "fsdp", None), P("section", "fsdp", None), P(), P(), P(), P())
    out_specs = (P("section", "fsdp", None), P("section", "fsdp", None))
    return jax.shard_map(
        per_device, mesh=mesh, in_specs=in_specs, out_specs=out_specs, check_vma=False
    )
```

```python
import math

import jax
import jax.numpy as jnp
from jax import lax
from jax.experimental import pallas as pl
from jax.experimental.pallas import tpu as pltpu
from jax.sharding import PartitionSpec as P

HEAD_DIM = 128
MESH = pl.DeviceIdType.MESH
NC = 8
NG = 4
TU = 8
SPLIT = 224


def body(oldsec, newsec, oldord, neword, freq, pieces, tokens, kv_out, shard_out,
         px, pc, og, cand, gb, wb, n2, sha, shb, xb, acc, ob, kvb, ct, st,
         pc_sem, rs, rr, zs, zr, xs, xr, ns, nr, shl, shs, shr,
         tl, tas, tar, ts, tr, tfs, tfr, osm, orm, kvs, xr1):
    rows = pieces.shape[1]
    cw = pieces.shape[2] // NC
    gw = pieces.shape[2] // NG
    per = NC // NG
    tok_rows, width = tokens.shape
    layers = oldsec.shape[0]
    s = lax.axis_index("section")
    m = lax.axis_index("fsdp")
    y = s // 2
    c = s % 2
    j = m // 16
    x = (m // 4) % 4
    z = m % 4
    h = z % 2
    zh = z // 2
    prob = (j + zh) % 2
    is_a = c == prob
    is_b = c != prob
    alone = jnp.logical_and(c == j, zh == 0)
    not_alone = jnp.logical_or(c != j, zh != 0)

    def dev(yy, cc, jj, xx, zz):
        return (2 * yy + cc, jj * 16 + xx * 4 + zz)

    core_dev = dev(y, 1 - c, j, x, z)
    cross_dev = [dev(1 - y, k, 1 - j, x, z) for k in range(2)]
    zf = (z + 2) % 4
    xp, xm, xf = (x + 1) % 4, (x + 3) % 4, (x + 2) % 4
    xp_dev, xm_dev = (dev(y, c, j, xx, z) for xx in (xp, xm))

    def remote(src, dst, send, recv, device):
        return pltpu.make_async_remote_copy(
            src_ref=src, dst_ref=dst, send_sem=send, recv_sem=recv,
            device_id=device, device_id_type=MESH)

    def arrived(dst, send, recv, device):
        remote(dst, dst, send, recv, device).wait_recv()

    def pc_copy(i):
        to = px.at[x] if i == 0 else pc.at[i]
        return pltpu.make_async_copy(pieces.at[:, :, pl.ds(i * cw, cw)], to, pc_sem.at[i])

    for i in range(NC):
        pc_copy(i).start()

    def layer_of(section):
        found = jnp.int32(0)
        for l in range(layers):
            found = found + jnp.where(newsec[l] == section, l, 0)
        return found

    def entry(table, layer):
        found = jnp.int32(0)
        for l in range(layers):
            found = found + jnp.where(layer == l, table(l), 0)
        return found

    high = jnp.int32(0)
    for l in range(layers):
        high = jnp.where(oldsec[l] == s, l, high)
    row_high = entry(lambda l: newsec[l], high) // 2
    source = [entry(lambda l: oldsec[l], layer_of(2 * s + k)) for k in range(2)]
    gl = layer_of(2 * (2 * y + prob) + h)
    gl_crossed = jnp.where(entry(lambda l: oldsec[l], gl) // 2 == y, 0, 1)
    gl_old = entry(lambda l: oldord[0, l], gl)
    gl_new = entry(lambda l: neword[0, l], gl)
    gl_turn = (jnp.where(gl_old == gl_new, 0, 1) + gl_crossed + j + c) % 2
    is_key = gl_old == (c + gl_crossed) % 2
    ol = layer_of(2 * s + h)
    ol_crossed = jnp.where(entry(lambda l: oldsec[l], ol) // 2 == y, 0, 1)
    key_at = (entry(lambda l: oldord[0, l], ol) + ol_crossed) % 2

    barrier = pltpu.get_barrier_semaphore()
    partners = cross_dev + [xp_dev, xm_dev]
    for n in range(1, 16):
        partners.append(dev(y, (c + n) % 2, (j + n // 2) % 2, x, (z + n // 4) % 4))
    for device in partners:
        pl.semaphore_signal(barrier, inc=1, device_id=device, device_id_type=MESH)
    pl.semaphore_wait(barrier, len(partners))

    tok_step = width // (2 * TU)
    quarter = width // 4

    slots = [x, xm, xp, xf]

    def tok_cols(u, a):
        start = slots[u // 2] * quarter + (2 * a + u % 2) * tok_step
        return pl.ds(pl.multiple_of(start, tok_step), tok_step)

    def tok_send(v):
        u, a = v // 2, v % 2
        cols = tok_cols(u, a)
        parts = [(pl.ds(0, SPLIT), dev(y, a, 1 - j, x, z)),
                 (pl.ds(SPLIT, tok_rows - SPLIT), dev(y, a, j, x, zf))]
        return [remote(tokens.at[part, cols], xb.at[1, part, cols], ts.at[0], tr.at[u, k], device)
                for k, (part, device) in enumerate(parts)]

    def tok_here(u):
        cols = tok_cols(u, c)
        for k, part in enumerate((pl.ds(0, SPLIT), pl.ds(SPLIT, tok_rows - SPLIT))):
            arrived(xb.at[1, part, cols], tfs.at[0], tr.at[u, k], core_dev)

    def tok_pass(u):
        cols = tok_cols(u, c)
        return remote(xb.at[1, :, cols], xb.at[1, :, cols], tfs.at[0], tfr.at[u], core_dev)

    def tok_other(u):
        cols = tok_cols(u, 1 - c)
        return remote(xb.at[1, :, cols], xb.at[1, :, cols], tfs.at[0], tfr.at[u], core_dev)

    def tok_core(k):
        cols = pl.ds(k * quarter, quarter)
        return remote(tokens.at[:, cols], xb.at[0, :, cols], tas.at[0], tar.at[k], core_dev)

    tok_local = pltpu.make_async_copy(tokens, xb.at[0], tl.at[0])
    tok_next = [0]

    def send_tokens(count):
        take = range(tok_next[0], min(tok_next[0] + count, 2 * TU))
        tok_next[0] += len(take)

        @pl.when(is_b)
        def _():
            for v in take:
                for copy in tok_send(v):
                    copy.start()

    def relay_copies(e):
        return [remote(og.at[e, k], cand.at[e, s], rs.at[0],
                       rr.at[e, 0] if k == 0 else rr.at[e, 1 + c], device)
                for k, device in enumerate([core_dev] + cross_dev)]

    relay_rows = [2 * y + 1 - c, 2 * (1 - y), 2 * (1 - y) + 1]
    first_entries = [0] + [NC + k for k in range(3)]

    def relay(e, of):
        def tile(t, carry):
            part = pl.ds(pl.multiple_of(t * 128, 128), 128)
            low_rows, high_rows = of(0, part), of(1, part)
            for k in range(3):
                og[e, k, part, :] = jnp.where(row_high == relay_rows[k], high_rows, low_rows)
            cand[e, s, part, :] = jnp.where(row_high == s, high_rows, low_rows)
            return carry

        lax.fori_loop(0, rows // 128, tile, 0)
        for copy in relay_copies(e):
            copy.start()

    def relay_send(i):
        pc_copy(i).wait()
        relay(i, lambda a, part: pc[i, a, part, :])

    def relay_first(b):
        relay(first_entries[b], lambda a, part: px[slots[b], a, part, :])

    def entry_of(i, slot):
        return first_entries[slot] if i == 0 else i

    def place(slot, zz):
        return pl.ds(pl.multiple_of((slots[slot] * 4 + zz) * rows, rows), rows)

    def spread(i, slot):
        copies = []
        for k in range(2):
            src = gb.at[slots[slot], k] if i == 0 else pc.at[i, k]
            target = 2 * ((c + j) % 2) + k
            for far in (1, 0):
                device = dev(y, j, (j + far) % 2, x, (target + 2 * far) % 4)
                copy = remote(src, wb.at[i, place(slot, z)], zs.at[far + 2 * (i == 0)],
                              zr.at[entry_of(i, slot), z], device)
                here = jnp.logical_and(alone, h == k)
                copies.append((copy, None if far else jnp.logical_not(here)))
        return copies

    def spread_each(i, slot, act):
        for copy, needed in spread(i, slot):
            if needed is None:
                act(copy)
            else:
                @pl.when(needed)
                def _():
                    act(copy)

    def spread_start(i, slot):
        spread_each(i, slot, lambda copy: copy.start())

    def spread_arrived(i, slot):
        for n in range(1, 4):
            zz = (z + n) % 4
            arrived(wb.at[i, place(slot, zz)], zs.at[0], zr.at[entry_of(i, slot), zz], core_dev)

        @pl.when(not_alone)
        def _():
            arrived(wb.at[i, place(slot, z)], zs.at[0], zr.at[entry_of(i, slot), z], core_dev)

    def choose_from(e, i, slot, to):
        arrived(cand.at[e, 2 * y + 1 - c], rs.at[0], rr.at[e, 0], core_dev)
        for k in range(2):
            arrived(cand.at[e, 2 * (1 - y) + k], rs.at[0], rr.at[e, 1 + k], cross_dev[k])

        def tile(t, carry):
            part = pl.ds(pl.multiple_of(t * 128, 128), 128)
            four = [cand[e, k, part, :] for k in range(4)]
            for k in range(2):
                want = source[k]
                to[k, part, :] = jnp.where(want < 2, jnp.where(want == 0, four[0], four[1]),
                                           jnp.where(want == 2, four[2], four[3]))
            return carry

        lax.fori_loop(0, rows // 128, tile, 0)
        spread_start(i, slot)

        @pl.when(alone)
        def _():
            def keep(t, carry):
                part = pl.ds(pl.multiple_of(t * 128, 128), 128)
                here = pl.ds(pl.multiple_of((slots[slot] * 4 + z) * rows + t * 128, 128), 128)
                wb[i, here, :] = to[h, part, :]
                return carry

            lax.fori_loop(0, rows // 128, keep, 0)

    def choose(i):
        choose_from(i, i, 0, pc.at[i])

    def choose_first(b):
        choose_from(first_entries[b], 0, b, gb.at[slots[b]])

    def first_own_copies():
        mine = px.at[x]
        return [remote(mine, mine, xs.at[0], xr.at[0, 0], xp_dev),
                remote(mine, mine, xs.at[0], xr.at[0, 1], xm_dev)]

    def first_pass_copies():
        left, right = px.at[xm, 0], px.at[xp, 1]
        return [remote(left, left, xs.at[0], xr.at[0, 2], xp_dev),
                remote(right, right, xs.at[0], xr.at[0, 3], xm_dev)]

    def first_own():
        pc_copy(0).wait()
        for copy in first_own_copies():
            copy.start()

    def first_pass():
        arrived(px.at[xm], xs.at[0], xr.at[0, 0], xp_dev)
        arrived(px.at[xp], xs.at[0], xr.at[0, 1], xm_dev)
        for copy in first_pass_copies():
            copy.start()

    def first_far():
        arrived(px.at[xf, 0], xs.at[0], xr.at[0, 2], xp_dev)
        arrived(px.at[xf, 1], xs.at[0], xr.at[0, 3], xm_dev)

    def block(i, xx, first, count):
        return wb.at[i, pl.ds(pl.multiple_of(xx * 4 * rows + first, rows), count)]

    def own_copies(i):
        mine = block(i, x, 0, 4 * rows)
        return [remote(mine, mine, xs.at[1], xr.at[i, 0], xp_dev),
                remote(mine, mine, xs.at[1], xr.at[i, 1], xm_dev)]

    def pass_copies(i):
        left = block(i, xm, 0, 2 * rows)
        right = block(i, xp, 2 * rows, 2 * rows)
        return [remote(left, left, xs.at[1], xr.at[i, 2], xp_dev),
                remote(right, right, xs.at[1], xr.at[i, 3], xm_dev)]

    pair = pl.ds(pl.multiple_of((x * 4 + z // 2 * 2) * rows, rows), 2 * rows)

    def near_copy(i):
        return remote(wb.at[i, pair], n2.at[i], ns.at[0], nr.at[i], core_dev)

    def x_own(i):
        spread_arrived(i, 0)
        if i > 0:
            for copy in own_copies(i):
                copy.start()

        @pl.when(is_b)
        def _():
            near_copy(i).start()

    def own_pieces(zz):
        mine = wb.at[1, place(0, zz)]
        return [remote(mine, mine, xs.at[1], xr1.at[0, zz], xp_dev),
                remote(mine, mine, xs.at[1], xr1.at[1, zz], xm_dev)]

    def x_arrived(i, side, slot, device):
        if i == 1:
            for zz in range(4):
                arrived(wb.at[1, place(slot, zz)], xs.at[1], xr1.at[side, zz], device)
        else:
            arrived(block(i, slots[slot], 0, 4 * rows), xs.at[1], xr.at[i, side], device)

    def x_own_first():
        for n in (0, 1, 3, 2):
            zz = (z + n) % 4
            if n == 0:
                @pl.when(not_alone)
                def _():
                    arrived(wb.at[1, place(0, z)], zs.at[0], zr.at[1, z], core_dev)
            else:
                arrived(wb.at[1, place(0, zz)], zs.at[0], zr.at[1, zz], core_dev)
            for copy in own_pieces(zz):
                copy.start()

        @pl.when(is_b)
        def _():
            near_copy(1).start()

    def x_pass(i):
        x_arrived(i, 0, 1, xp_dev)
        first, second = pass_copies(i)
        first.start()
        x_arrived(i, 1, 2, xm_dev)
        second.start()

    def far_arrived(i):
        if i == 0:
            for slot in (1, 2, 3):
                spread_arrived(i, slot)
            return
        arrived(block(i, xf, 0, 2 * rows), xs.at[1], xr.at[i, 2], xp_dev)
        arrived(block(i, xf, 2 * rows, 2 * rows), xs.at[1], xr.at[i, 3], xm_dev)

    def shard_local(i):
        return pltpu.make_async_copy(sha.at[i], shard_out.at[:, pl.ds(i * cw, cw)], shl.at[i])

    def shard_far(i):
        return remote(shb.at[i], shard_out.at[:, pl.ds(i * cw, cw)], shs.at[0], shr.at[0],
                      dev(y, c, 1 - j, x, z))

    def shard(i):
        @pl.when(is_a)
        def _():
            near_copy(i).wait_recv()

            def tile(t, carry):
                part = pl.ds(pl.multiple_of(t * 128, 128), 128)
                near = pl.ds(pl.multiple_of((x * 4 + z // 2 * 2) * rows + t * 128, 128), 128)
                mine = wb[i, near, :]
                other = n2[i, part, :]
                sha[i, part, :] = jnp.where(gl_turn == 0, mine, other)
                shb[i, part, :] = jnp.where(gl_turn == 0, other, mine)
                return carry

            lax.fori_loop(0, 2 * rows // 128, tile, 0)

    def shard_send(i):
        @pl.when(is_a)
        def _():
            shard_local(i).start()
            shard_far(i).start()

    def multiply(g, slots_now, xx, half):
        first = pl.multiple_of(xx * 4 * rows + half * 2 * rows, 2 * rows)
        ks = pl.ds(first, 2 * rows)
        weight = jnp.concatenate([wb[per * g + k, ks, :] for k in range(per)], axis=1)
        for slot in slots_now:
            acc[g, slot] += jnp.dot(xb[slot, :, ks], weight, preferred_element_type=jnp.float32)

    def clear(g):
        acc[g] = jnp.zeros(acc.shape[1:], acc.dtype)

    def near(g, slots_now, start, stop):
        def near_block(t, carry):
            b = t // 2
            multiply(g, slots_now, (x + 3 * b - b // 2 * 5) % 4, t % 2)
            return carry

        lax.fori_loop(2 * start, 2 * stop, near_block, 0)

    def far(g, slots_now):
        def far_block(t, carry):
            multiply(g, slots_now, xf, t)
            return carry

        lax.fori_loop(0, 2, far_block, 0)

    def finish(g, slot):
        def tile(t, carry):
            part = pl.ds(pl.multiple_of(t * 128, 128), 128)
            cosine = ct[slot, part, :]
            sine = st[slot, part, :]
            for head in range(gw // HEAD_DIM):
                cols = slice(head * HEAD_DIM, (head + 1) * HEAD_DIM)
                value = acc[g, slot, part, cols]
                turned = value * cosine + pltpu.roll(value, HEAD_DIM // 2, 1) * sine
                ob[g, slot, part, cols] = turned.astype(jnp.bfloat16)
            return carry

        lax.fori_loop(0, tok_rows // 128, tile, 0)

    def kv_part(g, q, part):
        return kvb.at[q, part, pl.ds(g * gw, gw)]

    all_rows = pl.ds(0, tok_rows)
    y_rows, z_rows = pl.ds(0, SPLIT), pl.ds(SPLIT, tok_rows - SPLIT)

    def out_near(g):
        return remote(ob.at[g, 0], kv_part(g, c, all_rows), osm.at[g, 0], orm.at[g, c], core_dev)

    def out_far(g):
        return [remote(ob.at[g, 1, y_rows], kv_part(g, c, y_rows), osm.at[g, 1], orm.at[g, c],
                       dev(y, prob, 1 - j, x, z)),
                remote(ob.at[g, 1, z_rows], kv_part(g, c, z_rows), osm.at[g, 2], orm.at[g, 2 + c],
                       dev(y, prob, j, x, zf))]

    def send_far(g):
        for copy in out_far(g):
            copy.start()

    def send_near(g):
        @pl.when(is_a)
        def _():
            def tile(t, carry):
                part = pl.ds(pl.multiple_of(t * 128, 128), 128)
                kvb[c, part, g * gw:(g + 1) * gw] = ob[g, 0, part, :]
                return carry

            lax.fori_loop(0, tok_rows // 128, tile, 0)

        @pl.when(is_b)
        def _():
            out_near(g).start()

    def stage(n):
        return cand.at[1 + n // 4, n % 4]

    def kv_copies(g):
        copies = []
        for n in range(2 * per):
            k, part = n // per, n % per
            cols = pl.ds(k * NG * gw + g * gw + part * cw, cw)
            copies.append(pltpu.make_async_copy(stage(2 * per * g + n), kv_out.at[:, cols],
                                                kvs.at[g, n]))
        return copies

    def collect(g):
        @pl.when(is_a)
        def _():
            arrived(kv_part(g, 1 - c, all_rows), osm.at[g, 0], orm.at[g, 1 - c], core_dev)

        @pl.when(is_b)
        def _():
            for q in range(2):
                arrived(kv_part(g, q, y_rows), osm.at[g, 0], orm.at[g, q], core_dev)
                arrived(kv_part(g, q, z_rows), osm.at[g, 0], orm.at[g, 2 + q], core_dev)

        def tile(t, carry):
            rows_now = pl.ds(pl.multiple_of(t * 128, 128), 128)
            for part in range(per):
                cols = slice(g * gw + part * cw, g * gw + (part + 1) * cw)
                first, second = kvb[0, rows_now, cols], kvb[1, rows_now, cols]
                stage(2 * per * g + part)[rows_now, :] = jnp.where(key_at == 0, first, second)
                stage(2 * per * g + per + part)[rows_now, :] = jnp.where(key_at == 0, second, first)
            return carry

        lax.fori_loop(0, tok_rows // 128, tile, 0)
        for copy in kv_copies(g):
            copy.start()

    def tables():
        first = m // 2 * tok_rows
        by_y = (m // 2 + 8) % 16 * tok_rows
        by_z = (m // 2 + 1 - 2 * zh) * tok_rows
        lane = lax.broadcasted_iota(jnp.int32, (64, HEAD_DIM), 1)
        row = lax.broadcasted_iota(jnp.int32, (64, HEAD_DIM), 0)

        def tile(t, carry):
            part = pl.ds(pl.multiple_of(t * 64, 64), 64)
            for slot in range(2):
                base = first if slot == 0 else jnp.where(t * 64 + row < SPLIT, by_y, by_z)
                position = (base + t * 64 + row).astype(jnp.float32)
                angle = position * freq[0:1, :]
                sine = jnp.sin(angle)
                sine = jnp.where(lane < HEAD_DIM // 2, -sine, sine)
                ct[slot, part, :] = jnp.where(is_key, jnp.cos(angle), 1.0)
                st[slot, part, :] = jnp.where(is_key, sine, 0.0)
            return carry

        lax.fori_loop(0, tok_rows // 64, tile, 0)

    def token_pass(u):
        tok_here(u)
        tok_pass(u).start()

    def token_other(b):
        for u in (2 * b, 2 * b + 1):
            tok_other(u).wait_recv()

    first_own()
    for i in range(1, NC):
        relay_send(i)
    send_tokens(1)
    choose(1)
    first_pass()
    choose(2)
    x_own_first()
    first_far()
    for b in range(4):
        relay_first(b)
    choose(3)
    x_own(2)

    @pl.when(is_a)
    def _():
        tok_local.start()
        for k in range(4):
            tok_core(k).start()

    choose(4)
    x_own(3)
    x_pass(1)
    choose(5)
    x_own(4)
    choose(6)
    x_own(5)
    choose(7)
    send_tokens(TU)
    x_own(6)
    x_pass(2)
    x_own(7)
    tables()

    @pl.when(is_a)
    def _():
        tok_local.wait()

    @pl.when(is_b)
    def _():
        for k in range(4):
            tok_core(k).wait_recv()

    for g in range(NG):
        clear(g)
    x_pass(3)
    for b in range(4):
        choose_first(b)
    send_tokens(2 * TU)
    near(1, (0,), 0, 3)
    token_pass(0)
    x_pass(4)
    token_pass(1)
    token_other(0)
    near(1, (1,), 0, 1)
    token_pass(2)
    token_pass(3)
    x_pass(5)
    token_other(1)
    near(1, (1,), 1, 2)
    near(2, (0,), 0, 3)
    near(2, (1,), 0, 2)
    x_pass(6)
    for i in range(1, 8):
        shard(i)
        shard_send(i)
    x_own(0)
    far_arrived(0)
    near(0, (0,), 0, 3)
    near(0, (1,), 0, 2)
    x_pass(7)
    near(3, (0,), 0, 3)
    shard(0)
    shard_send(0)
    token_pass(4)
    token_pass(5)
    token_other(2)
    near(0, (1,), 2, 3)
    near(1, (1,), 2, 3)
    near(2, (1,), 2, 3)
    near(3, (1,), 0, 3)
    far_arrived(1)
    far(0, (0,))
    far_arrived(2)
    far_arrived(3)
    far(1, (0,))
    token_pass(6)
    token_pass(7)
    token_other(3)
    for g in range(NG):
        if g >= 2:
            for k in range(per):
                far_arrived(per * g + k)
        far(g, (1,))
        finish(g, 1)
        send_far(g)
        if g >= 2:
            far(g, (0,))
        finish(g, 0)
        send_near(g)
    for g in range(NG):
        collect(g)

    def sent(src, send):
        remote(src, src, send, nr.at[0], core_dev).wait_send()

    later = pl.ds(1, NC - 1)
    sent(og, rs.at[0])
    sent(px.at[pl.ds(0, 3)], xs.at[0])
    sent(wb.at[later, pl.ds(0, 12 * rows)], xs.at[1])
    sent(pc.at[later], zs.at[1])
    sent(gb, zs.at[3])

    @pl.when(not_alone)
    def _():
        sent(pc.at[later], zs.at[0])
        sent(gb, zs.at[2])

    @pl.when(alone)
    def _():
        sent(pc.at[later, pl.ds(0, 1)], zs.at[0])
        sent(gb.at[:, pl.ds(0, 1)], zs.at[2])

    @pl.when(is_a)
    def _():
        sent(tokens, tas.at[0])
        for i in range(NC):
            shard_local(i).wait()
        sent(shb, shs.at[0])

    @pl.when(is_b)
    def _():
        sent(tokens, ts.at[0])
        sent(n2, ns.at[0])
        arrived(shard_out, shs.at[0], shr.at[0], core_dev)
        for g in range(NG):
            out_near(g).wait_send()

    sent(xb.at[1, :, pl.ds(0, 2 * quarter)], tfs.at[0])
    for g in range(NG):
        for copy in out_far(g):
            copy.wait_send()
        for copy in kv_copies(g):
            copy.wait()


def per_device(old_pieces, section_inputs, old_section_of, new_section_of, old_order, new_order):
    pieces = old_pieces[0]
    tokens = section_inputs[0]
    _, rows, kv_width = pieces.shape
    tok_rows, width = tokens.shape
    cw, gw = kv_width // NC, kv_width // NG

    half_dim = HEAD_DIM // 2
    freq_index = (jnp.arange(HEAD_DIM, dtype=jnp.int32) % half_dim).astype(jnp.float32)
    inverse_freq = jnp.exp(freq_index * (-2.0 * math.log(500000.0) / HEAD_DIM))
    freq = jnp.broadcast_to(inverse_freq[None, :], (8, HEAD_DIM))

    dma = pltpu.SemaphoreType.DMA
    bf, fl = jnp.bfloat16, jnp.float32
    hbm = pl.BlockSpec(memory_space=pltpu.HBM)
    vmem = pl.BlockSpec(memory_space=pltpu.VMEM)
    smem = pl.BlockSpec(memory_space=pltpu.SMEM)
    kv, shards = pl.pallas_call(
        body,
        out_shape=(jax.ShapeDtypeStruct((tok_rows, 2 * kv_width), bf),
                   jax.ShapeDtypeStruct((2 * rows, kv_width), bf)),
        in_specs=[smem] * 4 + [vmem] + [hbm] * 2,
        out_specs=(hbm, hbm),
        scratch_shapes=[
            pltpu.VMEM((4, 2, rows, cw), bf),
            pltpu.VMEM((NC, 2, rows, cw), bf),
            pltpu.VMEM((NC + 3, 3, rows, cw), bf),
            pltpu.VMEM((NC + 3, 4, rows, cw), bf),
            pltpu.VMEM((4, 2, rows, cw), bf),
            pltpu.VMEM((NC, width, cw), bf),
            pltpu.VMEM((NC, 2 * rows, cw), bf),
            pltpu.VMEM((NC, 2 * rows, cw), bf),
            pltpu.VMEM((NC, 2 * rows, cw), bf),
            pltpu.VMEM((2, tok_rows, width), bf),
            pltpu.VMEM((NG, 2, tok_rows, gw), fl),
            pltpu.VMEM((NG, 2, tok_rows, gw), bf),
            pltpu.VMEM((2, tok_rows, kv_width), bf),
            pltpu.VMEM((2, tok_rows, HEAD_DIM), fl),
            pltpu.VMEM((2, tok_rows, HEAD_DIM), fl),
            dma((NC,)), dma((1,)), dma((NC + 3, 3)),
            dma((4,)), dma((NC + 3, 4)), dma((2,)), dma((NC, 4)),
            dma((1,)), dma((NC,)), dma((NC,)), dma((1,)), dma((1,)),
            dma((1,)), dma((1,)), dma((4,)), dma((1,)), dma((TU, 2)), dma((1,)), dma((TU,)),
            dma((NG, 3)), dma((NG, 4)), dma((NG, 2 * NC // NG)),
            dma((2, 4)),
        ],
        compiler_params=pltpu.CompilerParams(
            collective_id=0, has_side_effects=True, vmem_limit_bytes=66_000_000),
    )(old_section_of, new_section_of, old_order.T, new_order.T, freq, pieces, tokens)

    return shards[None], kv[None]


def solution(mesh):
    in_specs = (P("section", None, "fsdp", None), P("section", "fsdp", None), P(), P(), P(), P())
    out_specs = (P("section", "fsdp", None), P("section", "fsdp", None))
    return jax.shard_map(
        per_device, mesh=mesh, in_specs=in_specs, out_specs=out_specs, check_vma=False
    )
```

```python
import math

import jax
import jax.numpy as jnp
from jax import lax
from jax.experimental import pallas as pl
from jax.experimental.pallas import tpu as pltpu
from jax.sharding import PartitionSpec as P

HEAD_DIM = 128
MESH = pl.DeviceIdType.MESH
NC = 8
NG = 4
TU = 8
SPLIT = 224


def body(oldsec, newsec, oldord, neword, freq, pieces, tokens, kv_out, shard_out,
         px, pc, og, cand, gb, wb, n2, sha, shb, xb, acc, ob, kvb, ct, st,
         pc_sem, rs, rr, zs, zr, xs, xr, ns, nr, shl, shs, shr,
         tl, tas, tar, ts, tr, tfs, tfr, osm, orm, kvs, xr1):
    rows = pieces.shape[1]
    cw = pieces.shape[2] // NC
    gw = pieces.shape[2] // NG
    per = NC // NG
    tok_rows, width = tokens.shape
    layers = oldsec.shape[0]
    s = lax.axis_index("section")
    m = lax.axis_index("fsdp")
    y = s // 2
    c = s % 2
    j = m // 16
    x = (m // 4) % 4
    z = m % 4
    h = z % 2
    zh = z // 2
    prob = (j + zh) % 2
    is_a = c == prob
    is_b = c != prob
    alone = jnp.logical_and(c == j, zh == 0)
    not_alone = jnp.logical_or(c != j, zh != 0)

    def dev(yy, cc, jj, xx, zz):
        return (2 * yy + cc, jj * 16 + xx * 4 + zz)

    core_dev = dev(y, 1 - c, j, x, z)
    cross_dev = [dev(1 - y, k, 1 - j, x, z) for k in range(2)]
    zf = (z + 2) % 4
    xp, xm, xf = (x + 1) % 4, (x + 3) % 4, (x + 2) % 4
    xp_dev, xm_dev = (dev(y, c, j, xx, z) for xx in (xp, xm))

    def remote(src, dst, send, recv, device):
        return pltpu.make_async_remote_copy(
            src_ref=src, dst_ref=dst, send_sem=send, recv_sem=recv,
            device_id=device, device_id_type=MESH)

    def arrived(dst, send, recv, device):
        remote(dst, dst, send, recv, device).wait_recv()

    def pc_copy(i):
        to = px.at[x] if i == 0 else pc.at[i]
        return pltpu.make_async_copy(pieces.at[:, :, pl.ds(i * cw, cw)], to, pc_sem.at[i])

    for i in range(NC):
        pc_copy(i).start()

    def layer_of(section):
        found = jnp.int32(0)
        for l in range(layers):
            found = found + jnp.where(newsec[l] == section, l, 0)
        return found

    def entry(table, layer):
        found = jnp.int32(0)
        for l in range(layers):
            found = found + jnp.where(layer == l, table(l), 0)
        return found

    high = jnp.int32(0)
    for l in range(layers):
        high = jnp.where(oldsec[l] == s, l, high)
    row_high = entry(lambda l: newsec[l], high) // 2
    source = [entry(lambda l: oldsec[l], layer_of(2 * s + k)) for k in range(2)]
    gl = layer_of(2 * (2 * y + prob) + h)
    gl_crossed = jnp.where(entry(lambda l: oldsec[l], gl) // 2 == y, 0, 1)
    gl_old = entry(lambda l: oldord[0, l], gl)
    gl_new = entry(lambda l: neword[0, l], gl)
    gl_turn = (jnp.where(gl_old == gl_new, 0, 1) + gl_crossed + j + c) % 2
    is_key = gl_old == (c + gl_crossed) % 2
    ol = layer_of(2 * s + h)
    ol_crossed = jnp.where(entry(lambda l: oldsec[l], ol) // 2 == y, 0, 1)
    key_at = (entry(lambda l: oldord[0, l], ol) + ol_crossed) % 2

    barrier = pltpu.get_barrier_semaphore()
    partners = cross_dev + [xp_dev, xm_dev]
    for n in range(1, 16):
        partners.append(dev(y, (c + n) % 2, (j + n // 2) % 2, x, (z + n // 4) % 4))
    for device in partners:
        pl.semaphore_signal(barrier, inc=1, device_id=device, device_id_type=MESH)
    pl.semaphore_wait(barrier, len(partners))

    tok_step = width // (2 * TU)
    quarter = width // 4

    slots = [x, xm, xp, xf]

    def tok_cols(u, a):
        start = slots[u // 2] * quarter + (2 * a + u % 2) * tok_step
        return pl.ds(pl.multiple_of(start, tok_step), tok_step)

    def tok_send(v):
        u, a = v // 2, v % 2
        cols = tok_cols(u, a)
        parts = [(pl.ds(0, SPLIT), dev(y, a, 1 - j, x, z)),
                 (pl.ds(SPLIT, tok_rows - SPLIT), dev(y, a, j, x, zf))]
        return [remote(tokens.at[part, cols], xb.at[1, part, cols], ts.at[0], tr.at[u], device)
                for k, (part, device) in enumerate(parts)]

    def tok_here(u):
        cols = tok_cols(u, c)
        arrived(xb.at[1, :, cols], tfs.at[0], tr.at[u], core_dev)

    def tok_pass(u):
        cols = tok_cols(u, c)
        return remote(xb.at[1, :, cols], xb.at[1, :, cols], tfs.at[0], tfr.at[u], core_dev)

    def tok_other(u):
        cols = tok_cols(u, 1 - c)
        return remote(xb.at[1, :, cols], xb.at[1, :, cols], tfs.at[0], tfr.at[u], core_dev)

    def tok_core(k):
        cols = pl.ds(k * quarter, quarter)
        return remote(tokens.at[:, cols], xb.at[0, :, cols], tas.at[0], tar.at[k], core_dev)

    tok_local = pltpu.make_async_copy(tokens, xb.at[0], tl.at[0])
    tok_next = [0]

    def send_tokens(count):
        take = range(tok_next[0], min(tok_next[0] + count, 2 * TU))
        tok_next[0] += len(take)

        @pl.when(is_b)
        def _():
            for v in take:
                for copy in tok_send(v):
                    copy.start()

    def relay_copies(e):
        return [remote(og.at[e, k], cand.at[e, s], rs.at[0],
                       rr.at[e], device)
                for k, device in enumerate([core_dev] + cross_dev)]

    relay_rows = [2 * y + 1 - c, 2 * (1 - y), 2 * (1 - y) + 1]
    first_entries = [0] + [NC + k for k in range(3)]

    def relay(e, of):
        def tile(t, carry):
            part = pl.ds(pl.multiple_of(t * 128, 128), 128)
            low_rows, high_rows = of(0, part), of(1, part)
            for k in range(3):
                og[e, k, part, :] = jnp.where(row_high == relay_rows[k], high_rows, low_rows)
            cand[e, s, part, :] = jnp.where(row_high == s, high_rows, low_rows)
            return carry

        lax.fori_loop(0, rows // 128, tile, 0)
        for copy in relay_copies(e):
            copy.start()

    def relay_send(i):
        pc_copy(i).wait()
        relay(i, lambda a, part: pc[i, a, part, :])

    def relay_first(b):
        relay(first_entries[b], lambda a, part: px[slots[b], a, part, :])

    def entry_of(i, slot):
        return first_entries[slot] if i == 0 else i

    def place(slot, zz):
        return pl.ds(pl.multiple_of((slots[slot] * 4 + zz) * rows, rows), rows)

    def spread(i, slot):
        copies = []
        for k in range(2):
            src = gb.at[slots[slot], k] if i == 0 else pc.at[i, k]
            target = 2 * ((c + j) % 2) + k
            for far in (1, 0):
                device = dev(y, j, (j + far) % 2, x, (target + 2 * far) % 4)
                copy = remote(src, wb.at[i, place(slot, z)], zs.at[far + 2 * (i == 0)],
                              zr.at[entry_of(i, slot), z], device)
                here = jnp.logical_and(alone, h == k)
                copies.append((copy, None if far else jnp.logical_not(here)))
        return copies

    def spread_each(i, slot, act):
        for copy, needed in spread(i, slot):
            if needed is None:
                act(copy)
            else:
                @pl.when(needed)
                def _():
                    act(copy)

    def spread_start(i, slot):
        spread_each(i, slot, lambda copy: copy.start())

    def spread_arrived(i, slot):
        for n in range(1, 4):
            zz = (z + n) % 4
            arrived(wb.at[i, place(slot, zz)], zs.at[0], zr.at[entry_of(i, slot), zz], core_dev)

        @pl.when(not_alone)
        def _():
            arrived(wb.at[i, place(slot, z)], zs.at[0], zr.at[entry_of(i, slot), z], core_dev)

    def choose_from(e, i, slot, to):
        arrived(og.at[e], rs.at[0], rr.at[e], core_dev)

        def tile(t, carry):
            part = pl.ds(pl.multiple_of(t * 128, 128), 128)
            four = [cand[e, k, part, :] for k in range(4)]
            for k in range(2):
                want = source[k]
                to[k, part, :] = jnp.where(want < 2, jnp.where(want == 0, four[0], four[1]),
                                           jnp.where(want == 2, four[2], four[3]))
            return carry

        lax.fori_loop(0, rows // 128, tile, 0)
        spread_start(i, slot)

        @pl.when(alone)
        def _():
            def keep(t, carry):
                part = pl.ds(pl.multiple_of(t * 128, 128), 128)
                here = pl.ds(pl.multiple_of((slots[slot] * 4 + z) * rows + t * 128, 128), 128)
                wb[i, here, :] = to[h, part, :]
                return carry

            lax.fori_loop(0, rows // 128, keep, 0)

    def choose(i):
        choose_from(i, i, 0, pc.at[i])

    def choose_first(b):
        choose_from(first_entries[b], 0, b, gb.at[slots[b]])

    def first_own_copies():
        mine = px.at[x]
        return [remote(mine, mine, xs.at[0], xr.at[0, 0], xp_dev),
                remote(mine, mine, xs.at[0], xr.at[0, 1], xm_dev)]

    def first_pass_copies():
        left, right = px.at[xm, 0], px.at[xp, 1]
        return [remote(left, left, xs.at[0], xr.at[0, 2], xp_dev),
                remote(right, right, xs.at[0], xr.at[0, 3], xm_dev)]

    def first_own():
        pc_copy(0).wait()
        for copy in first_own_copies():
            copy.start()

    def first_pass():
        arrived(px.at[xm], xs.at[0], xr.at[0, 0], xp_dev)
        arrived(px.at[xp], xs.at[0], xr.at[0, 1], xm_dev)
        for copy in first_pass_copies():
            copy.start()

    def first_far():
        arrived(px.at[xf, 0], xs.at[0], xr.at[0, 2], xp_dev)
        arrived(px.at[xf, 1], xs.at[0], xr.at[0, 3], xm_dev)

    def block(i, xx, first, count):
        return wb.at[i, pl.ds(pl.multiple_of(xx * 4 * rows + first, rows), count)]

    def own_copies(i):
        mine = block(i, x, 0, 4 * rows)
        return [remote(mine, mine, xs.at[1], xr.at[i, 0], xp_dev),
                remote(mine, mine, xs.at[1], xr.at[i, 1], xm_dev)]

    def pass_copies(i):
        left = block(i, xm, 0, 2 * rows)
        right = block(i, xp, 2 * rows, 2 * rows)
        return [remote(left, left, xs.at[1], xr.at[i, 2], xp_dev),
                remote(right, right, xs.at[1], xr.at[i, 3], xm_dev)]

    pair = pl.ds(pl.multiple_of((x * 4 + z // 2 * 2) * rows, rows), 2 * rows)

    def near_copy(i):
        return remote(wb.at[i, pair], n2.at[i], ns.at[0], nr.at[i], core_dev)

    def x_own(i):
        spread_arrived(i, 0)
        if i > 0:
            for copy in own_copies(i):
                copy.start()

        @pl.when(is_b)
        def _():
            near_copy(i).start()

    def own_pieces(zz):
        mine = wb.at[1, place(0, zz)]
        return [remote(mine, mine, xs.at[1], xr1.at[0, zz], xp_dev),
                remote(mine, mine, xs.at[1], xr1.at[1, zz], xm_dev)]

    def x_arrived(i, side, slot, device):
        if i == 1:
            for zz in range(4):
                arrived(wb.at[1, place(slot, zz)], xs.at[1], xr1.at[side, zz], device)
        else:
            arrived(block(i, slots[slot], 0, 4 * rows), xs.at[1], xr.at[i, side], device)

    def x_own_first():
        for n in (0, 1, 3, 2):
            zz = (z + n) % 4
            if n == 0:
                @pl.when(not_alone)
                def _():
                    arrived(wb.at[1, place(0, z)], zs.at[0], zr.at[1, z], core_dev)
            else:
                arrived(wb.at[1, place(0, zz)], zs.at[0], zr.at[1, zz], core_dev)
            for copy in own_pieces(zz):
                copy.start()

        @pl.when(is_b)
        def _():
            near_copy(1).start()

    def x_pass(i):
        x_arrived(i, 0, 1, xp_dev)
        first, second = pass_copies(i)
        first.start()
        x_arrived(i, 1, 2, xm_dev)
        second.start()

    def far_arrived(i):
        if i == 0:
            for slot in (1, 2, 3):
                spread_arrived(i, slot)
            return
        arrived(block(i, xf, 0, 2 * rows), xs.at[1], xr.at[i, 2], xp_dev)
        arrived(block(i, xf, 2 * rows, 2 * rows), xs.at[1], xr.at[i, 3], xm_dev)

    def shard_local(i):
        return pltpu.make_async_copy(sha.at[i], shard_out.at[:, pl.ds(i * cw, cw)], shl.at[i])

    def shard_far(i):
        return remote(shb.at[i], shard_out.at[:, pl.ds(i * cw, cw)], shs.at[0], shr.at[0],
                      dev(y, c, 1 - j, x, z))

    def shard(i):
        @pl.when(is_a)
        def _():
            near_copy(i).wait_recv()

            def tile(t, carry):
                part = pl.ds(pl.multiple_of(t * 128, 128), 128)
                near = pl.ds(pl.multiple_of((x * 4 + z // 2 * 2) * rows + t * 128, 128), 128)
                mine = wb[i, near, :]
                other = n2[i, part, :]
                sha[i, part, :] = jnp.where(gl_turn == 0, mine, other)
                shb[i, part, :] = jnp.where(gl_turn == 0, other, mine)
                return carry

            lax.fori_loop(0, 2 * rows // 128, tile, 0)

    def shard_send(i):
        @pl.when(is_a)
        def _():
            shard_local(i).start()
            shard_far(i).start()

    def multiply(g, slots_now, xx, half):
        first = pl.multiple_of(xx * 4 * rows + half * 2 * rows, 2 * rows)
        ks = pl.ds(first, 2 * rows)
        weight = jnp.concatenate([wb[per * g + k, ks, :] for k in range(per)], axis=1)
        for slot in slots_now:
            acc[g, slot] += jnp.dot(xb[slot, :, ks], weight, preferred_element_type=jnp.float32)

    def clear(g):
        acc[g] = jnp.zeros(acc.shape[1:], acc.dtype)

    def near(g, slots_now, start, stop):
        def near_block(t, carry):
            b = t // 2
            multiply(g, slots_now, (x + 3 * b - b // 2 * 5) % 4, t % 2)
            return carry

        lax.fori_loop(2 * start, 2 * stop, near_block, 0)

    def far(g, slots_now):
        def far_block(t, carry):
            multiply(g, slots_now, xf, t)
            return carry

        lax.fori_loop(0, 2, far_block, 0)

    def finish(g, slot):
        def tile(t, carry):
            part = pl.ds(pl.multiple_of(t * 128, 128), 128)
            cosine = ct[slot, part, :]
            sine = st[slot, part, :]
            for head in range(gw // HEAD_DIM):
                cols = slice(head * HEAD_DIM, (head + 1) * HEAD_DIM)
                value = acc[g, slot, part, cols]
                turned = value * cosine + pltpu.roll(value, HEAD_DIM // 2, 1) * sine
                ob[g, slot, part, cols] = turned.astype(jnp.bfloat16)
            return carry

        lax.fori_loop(0, tok_rows // 128, tile, 0)

    def kv_part(g, q, part):
        return kvb.at[q, part, pl.ds(g * gw, gw)]

    all_rows = pl.ds(0, tok_rows)
    y_rows, z_rows = pl.ds(0, SPLIT), pl.ds(SPLIT, tok_rows - SPLIT)

    def out_near(g):
        return remote(ob.at[g, 0], kv_part(g, c, all_rows), osm.at[g, 0], orm.at[g], core_dev)

    def out_far(g):
        return [remote(ob.at[g, 1, y_rows], kv_part(g, c, y_rows), osm.at[g, 1], orm.at[g],
                       dev(y, prob, 1 - j, x, z)),
                remote(ob.at[g, 1, z_rows], kv_part(g, c, z_rows), osm.at[g, 2], orm.at[g],
                       dev(y, prob, j, x, zf))]

    def send_far(g):
        for copy in out_far(g):
            copy.start()

    def send_near(g):
        @pl.when(is_a)
        def _():
            def tile(t, carry):
                part = pl.ds(pl.multiple_of(t * 128, 128), 128)
                kvb[c, part, g * gw:(g + 1) * gw] = ob[g, 0, part, :]
                return carry

            lax.fori_loop(0, tok_rows // 128, tile, 0)

        @pl.when(is_b)
        def _():
            out_near(g).start()

    def stage(n):
        return cand.at[1 + n // 4, n % 4]

    def kv_copies(g):
        copies = []
        for n in range(2 * per):
            k, part = n // per, n % per
            cols = pl.ds(k * NG * gw + g * gw + part * cw, cw)
            copies.append(pltpu.make_async_copy(stage(2 * per * g + n), kv_out.at[:, cols],
                                                kvs.at[g, n]))
        return copies

    def collect(g):
        @pl.when(is_a)
        def _():
            arrived(kv_part(g, 1 - c, all_rows), osm.at[g, 0], orm.at[g], core_dev)

        @pl.when(is_b)
        def _():
            arrived(kvb.at[:, :, pl.ds(g * gw, gw)], osm.at[g, 0], orm.at[g], core_dev)

        def tile(t, carry):
            rows_now = pl.ds(pl.multiple_of(t * 128, 128), 128)
            for part in range(per):
                cols = slice(g * gw + part * cw, g * gw + (part + 1) * cw)
                first, second = kvb[0, rows_now, cols], kvb[1, rows_now, cols]
                stage(2 * per * g + part)[rows_now, :] = jnp.where(key_at == 0, first, second)
                stage(2 * per * g + per + part)[rows_now, :] = jnp.where(key_at == 0, second, first)
            return carry

        lax.fori_loop(0, tok_rows // 128, tile, 0)
        for copy in kv_copies(g):
            copy.start()

    def tables():
        first = m // 2 * tok_rows
        by_y = (m // 2 + 8) % 16 * tok_rows
        by_z = (m // 2 + 1 - 2 * zh) * tok_rows
        lane = lax.broadcasted_iota(jnp.int32, (64, HEAD_DIM), 1)
        row = lax.broadcasted_iota(jnp.int32, (64, HEAD_DIM), 0)

        def tile(t, carry):
            part = pl.ds(pl.multiple_of(t * 64, 64), 64)
            for slot in range(2):
                base = first if slot == 0 else jnp.where(t * 64 + row < SPLIT, by_y, by_z)
                position = (base + t * 64 + row).astype(jnp.float32)
                angle = position * freq[0:1, :]
                sine = jnp.sin(angle)
                sine = jnp.where(lane < HEAD_DIM // 2, -sine, sine)
                ct[slot, part, :] = jnp.where(is_key, jnp.cos(angle), 1.0)
                st[slot, part, :] = jnp.where(is_key, sine, 0.0)
            return carry

        lax.fori_loop(0, tok_rows // 64, tile, 0)

    def token_pass(u):
        tok_here(u)
        tok_pass(u).start()

    def token_other(b):
        for u in (2 * b, 2 * b + 1):
            tok_other(u).wait_recv()

    first_own()
    for i in range(1, NC):
        relay_send(i)
    send_tokens(1)
    choose(1)
    first_pass()
    choose(2)
    x_own_first()
    first_far()
    for b in range(4):
        relay_first(b)
    choose(3)
    x_own(2)

    @pl.when(is_a)
    def _():
        tok_local.start()
        for k in range(4):
            tok_core(k).start()

    choose(4)
    x_own(3)
    x_pass(1)
    choose(5)
    x_own(4)
    choose(6)
    x_own(5)
    choose(7)
    send_tokens(TU)
    x_own(6)
    x_pass(2)
    x_own(7)
    tables()

    @pl.when(is_a)
    def _():
        tok_local.wait()

    @pl.when(is_b)
    def _():
        for k in range(4):
            tok_core(k).wait_recv()

    for g in range(NG):
        clear(g)
    x_pass(3)
    for b in range(4):
        choose_first(b)
    send_tokens(2 * TU)
    near(1, (0,), 0, 3)
    token_pass(0)
    x_pass(4)
    token_pass(1)
    token_other(0)
    near(1, (1,), 0, 1)
    token_pass(2)
    token_pass(3)
    x_pass(5)
    token_other(1)
    near(1, (1,), 1, 2)
    near(2, (0,), 0, 3)
    near(2, (1,), 0, 2)
    x_pass(6)
    for i in range(1, 8):
        shard(i)
        shard_send(i)
    x_own(0)
    far_arrived(0)
    near(0, (0,), 0, 3)
    near(0, (1,), 0, 2)
    x_pass(7)
    near(3, (0,), 0, 3)
    shard(0)
    shard_send(0)
    token_pass(4)
    token_pass(5)
    token_other(2)
    near(0, (1,), 2, 3)
    near(1, (1,), 2, 3)
    near(2, (1,), 2, 3)
    near(3, (1,), 0, 3)
    far_arrived(1)
    far(0, (0,))
    far_arrived(2)
    far_arrived(3)
    far(1, (0,))
    token_pass(6)
    token_pass(7)
    token_other(3)
    for g in range(NG):
        if g >= 2:
            for k in range(per):
                far_arrived(per * g + k)
        far(g, (1,))
        finish(g, 1)
        send_far(g)
        if g >= 2:
            far(g, (0,))
        finish(g, 0)
        send_near(g)
    for g in range(NG):
        collect(g)

    def sent(src, send):
        remote(src, src, send, nr.at[0], core_dev).wait_send()

    later = pl.ds(1, NC - 1)
    sent(og, rs.at[0])
    sent(px.at[pl.ds(0, 3)], xs.at[0])
    sent(wb.at[later, pl.ds(0, 12 * rows)], xs.at[1])
    sent(pc.at[later], zs.at[1])
    sent(gb, zs.at[3])

    @pl.when(not_alone)
    def _():
        sent(pc.at[later], zs.at[0])
        sent(gb, zs.at[2])

    @pl.when(alone)
    def _():
        sent(pc.at[later, pl.ds(0, 1)], zs.at[0])
        sent(gb.at[:, pl.ds(0, 1)], zs.at[2])

    @pl.when(is_a)
    def _():
        sent(tokens, tas.at[0])
        for i in range(NC):
            shard_local(i).wait()
        sent(shb, shs.at[0])

    @pl.when(is_b)
    def _():
        sent(tokens, ts.at[0])
        sent(n2, ns.at[0])
        arrived(shard_out, shs.at[0], shr.at[0], core_dev)
        for g in range(NG):
            out_near(g).wait_send()

    sent(xb.at[1, :, pl.ds(0, 2 * quarter)], tfs.at[0])
    for g in range(NG):
        for copy in out_far(g):
            copy.wait_send()
        for copy in kv_copies(g):
            copy.wait()


def per_device(old_pieces, section_inputs, old_section_of, new_section_of, old_order, new_order):
    pieces = old_pieces[0]
    tokens = section_inputs[0]
    _, rows, kv_width = pieces.shape
    tok_rows, width = tokens.shape
    cw, gw = kv_width // NC, kv_width // NG

    half_dim = HEAD_DIM // 2
    freq_index = (jnp.arange(HEAD_DIM, dtype=jnp.int32) % half_dim).astype(jnp.float32)
    inverse_freq = jnp.exp(freq_index * (-2.0 * math.log(500000.0) / HEAD_DIM))
    freq = jnp.broadcast_to(inverse_freq[None, :], (8, HEAD_DIM))

    dma = pltpu.SemaphoreType.DMA
    bf, fl = jnp.bfloat16, jnp.float32
    hbm = pl.BlockSpec(memory_space=pltpu.HBM)
    vmem = pl.BlockSpec(memory_space=pltpu.VMEM)
    smem = pl.BlockSpec(memory_space=pltpu.SMEM)
    kv, shards = pl.pallas_call(
        body,
        out_shape=(jax.ShapeDtypeStruct((tok_rows, 2 * kv_width), bf),
                   jax.ShapeDtypeStruct((2 * rows, kv_width), bf)),
        in_specs=[smem] * 4 + [vmem] + [hbm] * 2,
        out_specs=(hbm, hbm),
        scratch_shapes=[
            pltpu.VMEM((4, 2, rows, cw), bf),
            pltpu.VMEM((NC, 2, rows, cw), bf),
            pltpu.VMEM((NC + 3, 3, rows, cw), bf),
            pltpu.VMEM((NC + 3, 4, rows, cw), bf),
            pltpu.VMEM((4, 2, rows, cw), bf),
            pltpu.VMEM((NC, width, cw), bf),
            pltpu.VMEM((NC, 2 * rows, cw), bf),
            pltpu.VMEM((NC, 2 * rows, cw), bf),
            pltpu.VMEM((NC, 2 * rows, cw), bf),
            pltpu.VMEM((2, tok_rows, width), bf),
            pltpu.VMEM((NG, 2, tok_rows, gw), fl),
            pltpu.VMEM((NG, 2, tok_rows, gw), bf),
            pltpu.VMEM((2, tok_rows, kv_width), bf),
            pltpu.VMEM((2, tok_rows, HEAD_DIM), fl),
            pltpu.VMEM((2, tok_rows, HEAD_DIM), fl),
            dma((NC,)), dma((1,)), dma((NC + 3,)),
            dma((4,)), dma((NC + 3, 4)), dma((2,)), dma((NC, 4)),
            dma((1,)), dma((NC,)), dma((NC,)), dma((1,)), dma((1,)),
            dma((1,)), dma((1,)), dma((4,)), dma((1,)), dma((TU,)), dma((1,)), dma((TU,)),
            dma((NG, 3)), dma((NG,)), dma((NG, 2 * NC // NG)),
            dma((2, 4)),
        ],
        compiler_params=pltpu.CompilerParams(
            collective_id=0, has_side_effects=True, vmem_limit_bytes=66_000_000),
    )(old_section_of, new_section_of, old_order.T, new_order.T, freq, pieces, tokens)

    return shards[None], kv[None]


def solution(mesh):
    in_specs = (P("section", None, "fsdp", None), P("section", "fsdp", None), P(), P(), P(), P())
    out_specs = (P("section", "fsdp", None), P("section", "fsdp", None))
    return jax.shard_map(
        per_device, mesh=mesh, in_specs=in_specs, out_specs=out_specs, check_vma=False
    )
```
